8 devices in a mesh: sweep: 1 (over z), ent: 8 (over y, x, core).
Axes of the slice: x: 2, y: 2, z: 1, core: 2. Of those that a mesh axis runs over, the one named last changes fastest.
Arguments:
- ent_table: float32 [65536, 400], P(('sweep', 'ent'))
- ada_state: float32 [65536], P(('sweep', 'ent'))
- rel_table: float32 [237, 400], P('sweep')
- head_idx: int32 [8, 6, 1024], P(('sweep', 'ent'))
- tail_idx: int32 [8, 6, 1024], P(('sweep', 'ent'))
- rel_idx: int32 [8, 6, 1024], P(('sweep', 'ent'))
- neg_idx: int32 [8, 6, 256], P(('sweep', 'ent'))
- edge_mask: int32 [8, 6, 1024], P(('sweep', 'ent'))
Outputs:
- output 1: float32 [65536, 400], P(('sweep', 'ent'))
- output 2: float32 [65536], P(('sweep', 'ent'))
- output 3: float32 [237, 400], P('sweep')
- output 4: float32 [8, 6], P(('sweep', 'ent'))
All inputs are finite; a program needn't handle non-finite values.
Results may differ from the reference program's by a relative error of at most 0.00260891.
Values are sent between devices in bfloat16 or wider.
A program may use at most 1 GiB of HBM per device.

```python
import jax
import jax.numpy as jnp
from jax import lax

EMB_DIM = 400
REL_COUNT = 237
NEG_COUNT = 256
EDGE_COUNT = 1024
PART_ROWS = 8192
ROUNDS = 6
ENT_DEVS = 8

LEARN_RATE = 0.25
ADA_EPS = 1e-10
HOT_ROWS = PART_ROWS // 32
HOT_RELS = (REL_COUNT + 7) // 8


def draw_rows(key, shape, limit, hot_count):
    key_pick, key_wide, key_hot = jax.random.split(key, 3)
    hot_pick = jax.random.randint(key_pick, shape, 0, 2)
    wide_ids = jax.random.randint(key_wide, shape, 0, limit)
    hot_ids = jax.random.randint(key_hot, shape, 0, hot_count)
    picked = jnp.where(hot_pick == 1, hot_ids, wide_ids)
    return picked.at[0, 0, 0].set(limit - 1).astype(jnp.int32)


def setup_inputs(seed: int = 0, part: int = 0) -> dict:
    base_key = jax.random.key(seed)
    part_key = jax.random.fold_in(base_key, part)
    key_list = jax.random.split(part_key, 9)
    total_rows = ENT_DEVS * PART_ROWS
    edge_shape = (ENT_DEVS, ROUNDS, EDGE_COUNT)
    ent_table = jax.random.normal(key_list[0], (total_rows, EMB_DIM), jnp.float32)
    ada_state = jnp.exp2(-12.0 * jax.random.uniform(key_list[1], (total_rows,), jnp.float32)) / EMB_DIM
    rel_table = jax.random.normal(key_list[2], (REL_COUNT, EMB_DIM), jnp.float32) * (0.5 ** 0.5)
    head_idx = draw_rows(key_list[3], edge_shape, PART_ROWS, HOT_ROWS)
    tail_idx = draw_rows(key_list[4], edge_shape, PART_ROWS, HOT_ROWS)
    rel_idx = draw_rows(key_list[5], edge_shape, REL_COUNT, HOT_RELS)
    neg_idx = draw_rows(key_list[6], (ENT_DEVS, ROUNDS, NEG_COUNT), PART_ROWS, HOT_ROWS)
    fill_count = jax.random.randint(key_list[7], (ENT_DEVS, ROUNDS, 1), 0, EDGE_COUNT + 1)
    edge_mask = (jax.random.randint(key_list[8], edge_shape, 0, EDGE_COUNT) < fill_count).astype(jnp.int32)
    return {'ent_table': ent_table, 'ada_state': ada_state, 'rel_table': rel_table, 'head_idx': head_idx, 'tail_idx': tail_idx, 'rel_idx': rel_idx, 'neg_idx': neg_idx, 'edge_mask': edge_mask}


def bucket_grads(head_rows, tail_bf, neg_bf, rel_rows, weight):
    half_dim = EMB_DIM // 2
    score_scale = EMB_DIM ** -0.5
    h_re = head_rows[:, :half_dim]
    h_im = head_rows[:, half_dim:]
    r_re = rel_rows[:, :half_dim]
    r_im = rel_rows[:, half_dim:]
    query = jnp.concatenate([h_re * r_re - h_im * r_im, h_re * r_im + h_im * r_re], axis=1)
    query_bf = query.astype(jnp.bfloat16)
    tail_rows = tail_bf.astype(jnp.float32)
    pos_score = score_scale * jnp.sum(query * tail_rows, axis=1)
    neg_score = score_scale * jnp.dot(query_bf, neg_bf.T, preferred_element_type=jnp.float32)
    top_score = jnp.maximum(pos_score, jnp.max(neg_score, axis=1))
    pos_exp = jnp.exp(pos_score - top_score)
    neg_exp = jnp.exp(neg_score - top_score[:, None])
    denom_sum = pos_exp + jnp.sum(neg_exp, axis=1)
    weight_f = weight.astype(jnp.float32)
    loss_sum = jnp.sum(weight_f * (top_score + jnp.log(denom_sum) - pos_score))
    d_pos = weight_f * (pos_exp / denom_sum - 1.0)
    d_negs = ((weight_f / denom_sum)[:, None] * neg_exp).astype(jnp.bfloat16)
    d_query = score_scale * (d_pos[:, None] * tail_rows + jnp.dot(d_negs, neg_bf, preferred_element_type=jnp.float32))
    d_tail = score_scale * d_pos[:, None] * query
    d_neg = score_scale * jnp.dot(d_negs.T, query_bf, preferred_element_type=jnp.float32)
    dq_re = d_query[:, :half_dim]
    dq_im = d_query[:, half_dim:]
    d_head = jnp.concatenate([dq_re * r_re + dq_im * r_im, dq_im * r_re - dq_re * r_im], axis=1)
    d_rel = jnp.concatenate([dq_re * h_re + dq_im * h_im, dq_im * h_re - dq_re * h_im], axis=1)
    return loss_sum, d_head, d_tail, d_neg, d_rel


def adagrad_rows(table, state, row_grad):
    new_state = state + jnp.mean(row_grad * row_grad, axis=1)
    new_table = table - LEARN_RATE * row_grad / jnp.sqrt(new_state + ADA_EPS)[:, None]
    return new_table, new_state


def reference(ent_table, ada_state, rel_table, head_idx, tail_idx, rel_idx, neg_idx, edge_mask):
    dev_ids = jnp.arange(ENT_DEVS)
    head_base = dev_ids * PART_ROWS

    def round_body(carry, round_in):
        ent_cur, ada_cur, rel_cur, rel_acc = carry
        step, head_ids, tail_ids, rel_ids, neg_ids, mask_rows = round_in
        tail_base = ((dev_ids + step + 1) % ENT_DEVS) * PART_ROWS

        def one_bucket(bucket_in):
            head_off, tail_off, head_pick, tail_pick, rel_pick, neg_pick, mask_pick = bucket_in
            return bucket_grads(ent_cur[head_off + head_pick], ent_cur[tail_off + tail_pick].astype(jnp.bfloat16), ent_cur[tail_off + neg_pick].astype(jnp.bfloat16), rel_cur[rel_pick], mask_pick)

        loss_vals, d_head, d_tail, d_neg, d_rel = lax.map(one_bucket, (head_base, tail_base, head_ids, tail_ids, rel_ids, neg_ids, mask_rows))
        row_ids = jnp.concatenate([(head_base[:, None] + head_ids).reshape(-1), (tail_base[:, None] + tail_ids).reshape(-1), (tail_base[:, None] + neg_ids).reshape(-1)])
        row_grads = jnp.concatenate([d_head.reshape(-1, EMB_DIM), d_tail.reshape(-1, EMB_DIM), d_neg.reshape(-1, EMB_DIM)])
        row_grad = jax.ops.segment_sum(row_grads, row_ids, num_segments=ENT_DEVS * PART_ROWS)
        rel_grad = jax.ops.segment_sum(d_rel.reshape(-1, EMB_DIM), rel_ids.reshape(-1), num_segments=REL_COUNT)
        ent_cur, ada_cur = adagrad_rows(ent_cur, ada_cur, row_grad)
        rel_cur, rel_acc = adagrad_rows(rel_cur, rel_acc, rel_grad)
        return (ent_cur, ada_cur, rel_cur, rel_acc), loss_vals / EDGE_COUNT

    rel_zero = jnp.zeros((REL_COUNT,), jnp.float32)
    round_ins = (jnp.arange(ROUNDS), head_idx.transpose(1, 0, 2), tail_idx.transpose(1, 0, 2), rel_idx.transpose(1, 0, 2), neg_idx.transpose(1, 0, 2), edge_mask.transpose(1, 0, 2))
    final_state, loss_rounds = lax.scan(round_body, (ent_table, ada_state, rel_table, rel_zero), round_ins)
    return final_state[0], final_state[1], final_state[2], loss_rounds.T
```

```python
import functools

import jax
import jax.numpy as jnp
from jax import lax
from jax.experimental import pallas as pl
from jax.experimental.pallas import tpu as pltpu
from jax.sharding import PartitionSpec as P

LEARN_RATE = 0.25
ADA_EPS = 1e-10
LANES = 128
SUB = 32
CHUNK = 256
REL_ROWS = 256
VMEM = pltpu.VMEM
SMEM = pltpu.SMEM
F32 = jnp.float32
BF16 = jnp.bfloat16


def lane_iota(rows):
    return lax.broadcasted_iota(jnp.int32, (rows, LANES), 1)


def updated(e, a, emb_dim, lane):
    squares = (a[0] * a[0] + a[1] * a[1]) + (a[2] * a[2] + a[3] * a[3])
    state = jnp.sum(squares * (1.0 / emb_dim) + jnp.where(lane == LANES - 1, e[1], 0.0), axis=1, keepdims=True)
    scale = LEARN_RATE * lax.rsqrt(state + ADA_EPS)
    new = [e[c] - scale * a[c] for c in range(4)]
    new[1] = jnp.where(lane == LANES - 1, state, new[1])
    return new


def split3(x):
    hi = x.astype(BF16)
    rest = x - hi.astype(F32)
    mid = rest.astype(BF16)
    return hi, mid, (rest - mid.astype(F32)).astype(BF16)


def write_wire(buf, n, b, x, short, left, lane):
    base = b * SUB
    turned = pltpu.roll(x[3], short, axis=1)
    over = 2 * short - LANES
    rows = lambda part: pl.ds(pl.multiple_of(part * CHUNK + base, SUB), SUB)
    buf[n, rows(0), :] = x[0].astype(BF16)
    buf[n, rows(1), :] = x[2].astype(BF16)
    buf[n, rows(2), :] = jnp.where(lane < short, x[1], turned).astype(BF16)
    return left + pltpu.roll(jnp.where(lane < over, turned, 0.0), b * over, axis=1)


def read_wire(buf, n, b, short, left, lane):
    base = b * SUB
    rows = lambda part: pl.ds(pl.multiple_of(part * CHUNK + base, SUB), SUB)
    over = 2 * short - LANES
    x0 = buf[n, rows(0), :].astype(F32)
    x2 = buf[n, rows(1), :].astype(F32)
    mixed = buf[n, rows(2), :].astype(F32)
    x1 = jnp.where(lane < short, mixed, 0.0)
    kept = LANES - short
    tail = pltpu.roll(left, lax.rem(LANES + kept - b * over, LANES), axis=1)
    x3 = jnp.where(lane < kept, pltpu.roll(mixed, kept, axis=1), jnp.where(lane < short, tail, 0.0))
    return [x0, x1, x2, x3]


def load4(ref, at):
    return [ref[pl.ds(at, SUB), c, :] for c in range(4)]


def gather_rows(ref, acc, idx, start, rows_e, rows_a):
    for i in range(SUB):
        r = idx[start + i]
        rows_e[i] = ref[r]
        rows_a[i] = acc[r]


def dense_update(ent, acc, first, count, emb_dim):
    lane = lane_iota(SUB)
    zero = jnp.zeros((SUB, LANES), F32)

    def step(j, carry):
        at = pl.multiple_of((first + j) * SUB, SUB)
        new = updated(load4(ent, at), load4(acc, at), emb_dim, lane)
        for c in range(4):
            ent[pl.ds(at, SUB), c, :] = new[c]
            acc[pl.ds(at, SUB), c, :] = zero
        return carry

    lax.fori_loop(0, count, step, 0)


def main_kernel(shift, devs, emb_dim, head_idx, serve_idx, rel_idx, weight, rel_in, ent_in, acc_in,
                ent, acc, grads, rel_out, loss_out,
                rows_e, rows_a, rel_split, heads, rels, served, q_send, q_recv, dq_send, dq_recv, q_all, weights, scores,
                pos, d_pos, probs, d_neg, d_mix, d_split, rel_acc, rel_got, rel_half, rel_got1, rel_two, rel_got2, rel_sum,
                loss_send, loss_recv, q_ss, q_rs, d_ss, d_rs, r_ss, r_rs):
    edges = head_idx.shape[0]
    negs = serve_idx.shape[0] - edges
    chunks = edges // CHUNK
    subs = CHUNK // SUB
    half = emb_dim // 2
    short = half - LANES
    score_scale = emb_dim ** -0.5
    me = lax.axis_index("ent")
    owner = lax.rem(me + shift, devs)
    asker = lax.rem(me + devs - shift, devs)
    core = lax.rem(me, 2)
    x_at = lax.rem(me // 2, 2)
    y_at = me // 4
    mate = me + 1 - 2 * core
    x_mate = me + 2 - 4 * x_at
    y_mate = me + 4 - 8 * y_at
    lane = lane_iota(SUB)

    def copy_to(src, dst, send_sem, recv_sem, dev):
        return pltpu.make_async_remote_copy(src_ref=src, dst_ref=dst, send_sem=send_sem, recv_sem=recv_sem,
                                            device_id={"ent": dev}, device_id_type=pl.DeviceIdType.MESH)

    barrier = pltpu.get_barrier_semaphore()
    for dev in (owner, asker, mate, x_mate, y_mate):
        pl.semaphore_signal(barrier, inc=1, device_id={"ent": dev}, device_id_type=pl.DeviceIdType.MESH)

    def split_rel(j, carry):
        at = pl.ds(pl.multiple_of(j * SUB, SUB), SUB)
        for p, part in enumerate(split3(rel_in[at, :])):
            rel_split[at, 512 * p:512 * (p + 1)] = part
        return carry

    lax.fori_loop(0, REL_ROWS // SUB, split_rel, 0)

    def one_hot(n):
        ids = rel_idx[n:n + 1, :]
        return jnp.where(lax.broadcasted_iota(jnp.int32, (REL_ROWS, CHUNK), 0) == ids, 1.0, 0.0).astype(BF16)

    q_copies = []
    for n in range(chunks):
        picked = lax.dot_general(one_hot(n), rel_split[...], (((0,), (0,)), ((), ())), preferred_element_type=F32)
        rels[n * CHUNK:(n + 1) * CHUNK, :] = (picked[:, :512] + picked[:, 512:1024]) + picked[:, 1024:]

        def query(b, left, n=n):
            at = pl.multiple_of(n * CHUNK + b * SUB, SUB)
            gather_rows(ent_in, acc_in, head_idx, at, rows_e, rows_a)
            h = updated(load4(rows_e, 0), load4(rows_a, 0), emb_dim, lane)
            h[1] = jnp.where(lane < short, h[1], 0.0)
            r = [rels[pl.ds(at, SUB), LANES * c:LANES * (c + 1)] for c in range(4)]
            r[1] = jnp.where(lane < short, r[1], 0.0)
            for c in range(4):
                heads[pl.ds(at, SUB), LANES * c:LANES * (c + 1)] = h[c]
            q = [h[0] * r[0] - h[2] * r[2], h[1] * r[1] - h[3] * r[3], h[0] * r[2] + h[2] * r[0], h[1] * r[3] + h[3] * r[1]]
            return write_wire(q_send, n, b, q, short, left, lane)

        left = lax.fori_loop(0, subs, query, jnp.zeros((SUB, LANES), F32))
        q_send[n, 3 * CHUNK:, :] = left.astype(BF16)
        if n == 0:
            pl.semaphore_wait(barrier, 5)
        copy = copy_to(q_send.at[n], q_recv.at[n], q_ss.at[n], q_rs.at[n], owner)
        copy.start()
        q_copies.append(copy)

    def serve(j, carry):
        at = pl.multiple_of(j * SUB, SUB)
        gather_rows(ent_in, acc_in, serve_idx, at, rows_e, rows_a)
        t = updated(load4(rows_e, 0), load4(rows_a, 0), emb_dim, lane)
        t[1] = jnp.where(lane < short, t[1], 0.0)
        for c in range(4):
            served[pl.ds(at, SUB), LANES * c:LANES * (c + 1)] = t[c].astype(BF16)
        return carry

    lax.fori_loop(0, (edges + negs) // SUB, serve, 0)

    steps = ent.shape[0] // SUB
    loss = jnp.zeros((SUB, 1), F32)
    d_copies = []
    for n in range(chunks):
        dense_update(ent, acc, n * (steps // chunks), steps // chunks, emb_dim)
        for p in range(CHUNK // LANES):
            row = jnp.broadcast_to(weight[n:n + 1, LANES * p:LANES * (p + 1)], (LANES, LANES))
            weights[LANES * p:LANES * (p + 1), :] = jnp.transpose(row)
        copy_to(q_send.at[n], q_recv.at[n], q_ss.at[n], q_rs.at[n], owner).wait_recv()

        def arrive(b, carry, n=n):
            at = pl.multiple_of(b * SUB, SUB)
            q = read_wire(q_recv, n, b, short, q_recv[n, 3 * CHUNK:, :].astype(F32), lane)
            t = [served[pl.ds(pl.multiple_of(n * CHUNK + at, SUB), SUB), LANES * c:LANES * (c + 1)].astype(F32) for c in range(4)]
            pos[pl.ds(at, SUB), :] = score_scale * jnp.sum((q[0] * t[0] + q[1] * t[1]) + (q[2] * t[2] + q[3] * t[3]), axis=1, keepdims=True)
            for c in range(4):
                q_all[pl.ds(at, SUB), LANES * c:LANES * (c + 1)] = q[c].astype(BF16)
            return carry

        lax.fori_loop(0, subs, arrive, 0)
        scores[...] = lax.dot_general(q_all[...], served[edges:, :], (((1,), (1,)), ((), ())), preferred_element_type=F32)

        def soft(b, total):
            at = pl.ds(pl.multiple_of(b * SUB, SUB), SUB)
            s = score_scale * scores[at, :]
            p = pos[at, :]
            w = weights[at, 0:1]
            top = jnp.maximum(p, jnp.max(s, axis=1, keepdims=True))
            e = jnp.exp(s - top)
            pe = jnp.exp(p - top)
            denom = pe + jnp.sum(e, axis=1, keepdims=True)
            d_pos[at, :] = score_scale * (w * (pe / denom - 1.0))
            probs[at, :] = ((w / denom) * e).astype(BF16)
            return total + w * (top + jnp.log(denom) - p)

        loss = lax.fori_loop(0, subs, soft, loss)
        d_mix[...] = jnp.dot(probs[...], served[edges:, :], preferred_element_type=F32)
        part = lax.dot_general(probs[...], q_all[...], (((0,), (0,)), ((), ())), preferred_element_type=F32)
        if n == 0:
            d_neg[...] = part
        else:
            d_neg[...] += part

        def back(b, left, n=n):
            at = pl.multiple_of(b * SUB, SUB)
            dp = d_pos[pl.ds(at, SUB), :]
            dq = []
            for c in range(4):
                cols = slice(LANES * c, LANES * (c + 1))
                t = served[pl.ds(pl.multiple_of(n * CHUNK + at, SUB), SUB), cols].astype(F32)
                q = q_all[pl.ds(at, SUB), cols].astype(F32)
                dq.append(dp * t + score_scale * d_mix[pl.ds(at, SUB), cols])
                grads[pl.ds(pl.multiple_of(edges + n * CHUNK + at, SUB), SUB), c, :] = dp * q
            return write_wire(dq_send, n, b, dq, short, left, lane)

        left = lax.fori_loop(0, subs, back, jnp.zeros((SUB, LANES), F32))
        dq_send[n, 3 * CHUNK:, :] = left.astype(BF16)
        copy = copy_to(dq_send.at[n], dq_recv.at[n], d_ss.at[n], d_rs.at[n], asker)
        copy.start()
        d_copies.append(copy)

    loss_send[...] = jnp.broadcast_to(jnp.sum(loss, axis=0, keepdims=True), (8, LANES))
    loss_copy = copy_to(loss_send, loss_recv, r_ss.at[6], r_rs.at[6], asker)
    loss_copy.start()

    def neg_rows(b, carry):
        at = pl.multiple_of(b * SUB, SUB)
        for c in range(4):
            grads[pl.ds(pl.multiple_of(2 * edges + at, SUB), SUB), c, :] = score_scale * d_neg[pl.ds(at, SUB), LANES * c:LANES * (c + 1)]
        return carry

    lax.fori_loop(0, negs // SUB, neg_rows, 0)

    for n in range(chunks):
        copy_to(dq_send.at[n], dq_recv.at[n], d_ss.at[n], d_rs.at[n], asker).wait_recv()

        def own(b, carry, n=n):
            at = pl.multiple_of(n * CHUNK + b * SUB, SUB)
            dq = read_wire(dq_recv, n, b, short, dq_recv[n, 3 * CHUNK:, :].astype(F32), lane)
            h = [heads[pl.ds(at, SUB), LANES * c:LANES * (c + 1)] for c in range(4)]
            r = [rels[pl.ds(at, SUB), LANES * c:LANES * (c + 1)] for c in range(4)]
            r[1] = jnp.where(lane < short, r[1], 0.0)
            dh = [dq[0] * r[0] + dq[2] * r[2], dq[1] * r[1] + dq[3] * r[3], dq[2] * r[0] - dq[0] * r[2], dq[3] * r[1] - dq[1] * r[3]]
            dr = [dq[0] * h[0] + dq[2] * h[2], dq[1] * h[1] + dq[3] * h[3], dq[2] * h[0] - dq[0] * h[2], dq[3] * h[1] - dq[1] * h[3]]
            row = pl.ds(pl.multiple_of(b * SUB, SUB), SUB)
            for c in range(4):
                grads[pl.ds(at, SUB), c, :] = dh[c]
                for p, part in enumerate(split3(dr[c])):
                    d_split[row, 512 * p + LANES * c:512 * p + LANES * (c + 1)] = part
            return carry

        lax.fori_loop(0, subs, own, 0)
        part = jnp.dot(one_hot(n), d_split[...], preferred_element_type=F32)
        part = (part[:, :512] + part[:, 512:1024]) + part[:, 1024:]
        if n == 0:
            rel_acc[...] = part
        else:
            rel_acc[...] += part

    hrows = REL_ROWS // 2
    qrows = hrows // 2
    mine = pl.ds(pl.multiple_of(core * hrows, hrows), hrows)
    theirs = pl.ds(pl.multiple_of((1 - core) * hrows, hrows), hrows)
    c0 = copy_to(rel_acc.at[theirs], rel_got, r_ss.at[0], r_rs.at[0], mate)
    c0.start()
    c0.wait_recv()
    rel_half[...] = (rel_acc[mine, :] + rel_got[...]).astype(BF16)
    first, last = pl.ds(0, qrows), pl.ds(qrows, qrows)
    c1 = copy_to(rel_half.at[first], rel_got1.at[first], r_ss.at[1], r_rs.at[1], x_mate)
    c2 = copy_to(rel_half.at[last], rel_got1.at[last], r_ss.at[2], r_rs.at[2], y_mate)
    c1.start()
    c2.start()
    c1.wait_recv()
    rel_two[first, :] = (rel_half[first, :].astype(F32) + rel_got1[first, :].astype(F32)).astype(BF16)
    c3 = copy_to(rel_two.at[first], rel_got2.at[first], r_ss.at[3], r_rs.at[3], y_mate)
    c3.start()
    c2.wait_recv()
    rel_two[last, :] = (rel_half[last, :].astype(F32) + rel_got1[last, :].astype(F32)).astype(BF16)
    c4 = copy_to(rel_two.at[last], rel_got2.at[last], r_ss.at[4], r_rs.at[4], x_mate)
    c4.start()
    c3.wait_recv()
    c4.wait_recv()
    rel_sum[mine, :] = rel_two[...].astype(F32) + rel_got2[...].astype(F32)
    c5 = copy_to(rel_sum.at[mine], rel_sum.at[mine], r_ss.at[5], r_rs.at[5], mate)
    c5.start()
    c5.wait_recv()

    def rel_step(j, carry):
        at = pl.ds(pl.multiple_of(j * SUB, SUB), SUB)
        cols = [slice(LANES * c, LANES * (c + 1)) for c in range(4)]
        new = updated([rel_in[at, s] for s in cols], [rel_sum[at, s] for s in cols], emb_dim, lane)
        for c in range(4):
            rel_out[at, cols[c]] = new[c]
        return carry

    lax.fori_loop(0, REL_ROWS // SUB, rel_step, 0)
    loss_copy.wait_recv()
    loss_out[...] = loss_recv[...]
    for copy in q_copies + d_copies + [loss_copy, c0, c1, c2, c3, c4, c5]:
        copy.wait_send()


def scatter_kernel(idx, flags, grads, acc_in, acc):
    group = idx.shape[0] // flags.shape[0]

    def step(j, carry):
        at = j * group
        rows = [idx[at + i] for i in range(group)]

        @pl.when(flags[j] == 0)
        def _():
            new = [acc[rows[i]] + grads[at + i] for i in range(group)]
            for i in range(group):
                acc[rows[i]] = new[i]

        @pl.when(flags[j] != 0)
        def _():
            for i in range(group):
                acc[rows[i]] = acc[rows[i]] + grads[at + i]

        return carry

    lax.fori_loop(0, flags.shape[0], step, 0)


def enter_kernel(table, state, ent, acc, pad):
    blk = pl.program_id(0)
    cols = table.shape[1]
    half = table.shape[0] // 2
    short = half - LANES
    for j in range(cols // LANES):
        at = pl.ds(pl.multiple_of(blk * cols + j * LANES, LANES), LANES)
        lanes = slice(LANES * j, LANES * (j + 1))
        rows = lax.broadcasted_iota(jnp.int32, (LANES - short, LANES), 0)
        for c in range(4):
            first = (c // 2) * half
            if c % 2 == 0:
                piece = table[first:first + LANES, lanes]
            else:
                pad[0:short, :] = table[first + LANES:first + half, lanes]
                if c == 1:
                    pad[short:, :] = jnp.where(rows == LANES - short - 1, state[j:j + 1, :], 0.0)
                else:
                    pad[short:, :] = jnp.zeros((LANES - short, LANES), F32)
                piece = pad[...]
            ent[at, c, :] = jnp.transpose(piece)
            acc[at, c, :] = jnp.zeros((LANES, LANES), F32)


def leave_kernel(emb_dim, ent, acc, table, state):
    blk = pl.program_id(0)
    cols = table.shape[1]
    half = emb_dim // 2
    short = half - LANES
    lane = lane_iota(LANES)
    for j in range(cols // LANES):
        at = pl.ds(pl.multiple_of(blk * cols + j * LANES, LANES), LANES)
        lanes = slice(LANES * j, LANES * (j + 1))
        new = updated([ent[at, c, :] for c in range(4)], [acc[at, c, :] for c in range(4)], emb_dim, lane)
        for c in range(4):
            first = (c // 2) * half
            turned = jnp.transpose(new[c])
            if c % 2 == 0:
                table[first:first + LANES, lanes] = turned
            else:
                table[first + LANES:first + half, lanes] = turned[0:short, :]
                if c == 1:
                    state[j:j + 1, :] = turned[LANES - 1:LANES, :]


def solution(mesh):
    devs = mesh.shape["ent"]
    row_spec = P(("sweep", "ent"), None)
    state_spec = P(("sweep", "ent"))
    rel_spec = P("sweep", None)
    edge_spec = P(("sweep", "ent"), None, None)
    in_vmem = pl.BlockSpec(memory_space=VMEM)
    in_smem = pl.BlockSpec(memory_space=SMEM)
    hold = lambda x: pltpu.with_memory_space_constraint(x, VMEM)

    def per_device(ent_part, ada_part, rel_table, head_idx, tail_idx, rel_idx, neg_idx, edge_mask):
        rows, emb_dim = ent_part.shape
        rounds, edges = head_idx.shape[1:]
        negs = neg_idx.shape[2]
        rel_count = rel_table.shape[0]
        half = emb_dim // 2
        chunks = edges // CHUNK
        total = 2 * edges + negs
        packed = jax.ShapeDtypeStruct((rows, 4, LANES), F32)
        table_vmem = VMEM(packed.shape, F32)
        block = 1024 if rows % 1024 == 0 else LANES * 8

        served, masks = [], []
        for step in range(rounds):
            pairs = [(s, (s + step + 1) % devs) for s in range(devs)]
            packet = jnp.concatenate([tail_idx[0, step], neg_idx[0, step], edge_mask[0, step]])
            got = lax.ppermute(packet, "ent", pairs)
            served.append(got[:edges + negs])
            masks.append(got[edges + negs:].astype(F32).reshape(chunks, CHUNK))
        all_idx = [jnp.concatenate([head_idx[0, s], served[s]]) for s in range(rounds)]
        group = 8
        grouped = jnp.stack(all_idx).reshape(rounds, total // group, group)
        same = (grouped[:, :, :, None] == grouped[:, :, None, :]) & jnp.triu(jnp.ones((group, group), bool), 1)
        flags = jnp.any(same, axis=(2, 3)).astype(jnp.int32)

        ent, acc = pl.pallas_call(
            enter_kernel,
            grid=(rows // block,),
            out_shape=(table_vmem, table_vmem),
            in_specs=[pl.BlockSpec((emb_dim, block), lambda i: (0, i)), pl.BlockSpec((block // LANES, LANES), lambda i: (i, 0))],
            out_specs=(in_vmem, in_vmem),
            scratch_shapes=[VMEM((LANES, LANES), F32)],
            compiler_params=pltpu.CompilerParams(vmem_limit_bytes=24 << 20),
            name="enter",
        )(ent_part.T, ada_part.reshape(rows // LANES, LANES))
        fill = 2 * LANES - half
        rel = jnp.pad(rel_table.reshape(rel_count, 2, half), ((0, REL_ROWS - rel_count), (0, 0), (0, fill))).reshape(REL_ROWS, 4 * LANES)

        wire = (chunks, 3 * CHUNK + SUB, LANES)
        full = (edges, 4 * LANES)
        losses = []
        for step in range(rounds):
            ent, acc, grads, rel, loss = pl.pallas_call(
                functools.partial(main_kernel, step + 1, devs, emb_dim),
                out_shape=(table_vmem, table_vmem, VMEM((total, 4, LANES), F32), VMEM((REL_ROWS, 4 * LANES), F32), jax.ShapeDtypeStruct((8, LANES), F32)),
                in_specs=[in_smem, in_smem] + [in_vmem] * 5,
                out_specs=(in_vmem,) * 5,
                input_output_aliases={5: 0, 6: 1},
                scratch_shapes=[
                    VMEM((SUB, 4, LANES), F32), VMEM((SUB, 4, LANES), F32), VMEM((REL_ROWS, 12 * LANES), BF16), VMEM(full, F32), VMEM(full, F32),
                    VMEM((edges + negs, 4 * LANES), BF16), VMEM(wire, BF16), VMEM(wire, BF16), VMEM(wire, BF16), VMEM(wire, BF16),
                    VMEM((CHUNK, 4 * LANES), BF16), VMEM((CHUNK, LANES), F32), VMEM((CHUNK, negs), F32),
                    VMEM((CHUNK, 1), F32), VMEM((CHUNK, 1), F32), VMEM((CHUNK, negs), BF16), VMEM((negs, 4 * LANES), F32), VMEM((CHUNK, 4 * LANES), F32),
                    VMEM((CHUNK, 12 * LANES), BF16), VMEM((REL_ROWS, 4 * LANES), F32), VMEM((REL_ROWS // 2, 4 * LANES), F32),
                    VMEM((REL_ROWS // 2, 4 * LANES), BF16), VMEM((REL_ROWS // 2, 4 * LANES), BF16), VMEM((REL_ROWS // 2, 4 * LANES), BF16), VMEM((REL_ROWS // 2, 4 * LANES), BF16),
                    VMEM((REL_ROWS, 4 * LANES), F32), VMEM((8, LANES), F32), VMEM((8, LANES), F32),
                ] + [pltpu.SemaphoreType.DMA((chunks,))] * 4 + [pltpu.SemaphoreType.DMA((7,))] * 2,
                compiler_params=pltpu.CompilerParams(collective_id=step, has_side_effects=True, vmem_limit_bytes=26 << 20),
                name="train",
            )(head_idx[0, step], served[step], rel_idx[0, step].reshape(chunks, CHUNK), masks[step], rel if step == 0 else hold(rel), hold(ent), hold(acc))
            acc = pl.pallas_call(
                scatter_kernel,
                out_shape=table_vmem,
                in_specs=[in_smem, in_smem, in_vmem, in_vmem],
                out_specs=in_vmem,
                input_output_aliases={3: 0},
                compiler_params=pltpu.CompilerParams(vmem_limit_bytes=4 << 20),
                name="scatter",
            )(all_idx[step], flags[step], hold(grads), hold(acc))
            losses.append(loss[0, 0] / edges)

        table_t, state = pl.pallas_call(
            functools.partial(leave_kernel, emb_dim),
            grid=(rows // block,),
            out_shape=(jax.ShapeDtypeStruct((emb_dim, rows), F32), jax.ShapeDtypeStruct((rows // LANES, LANES), F32)),
            in_specs=[in_vmem, in_vmem],
            out_specs=(pl.BlockSpec((emb_dim, block), lambda i: (0, i)), pl.BlockSpec((block // LANES, LANES), lambda i: (i, 0))),
            compiler_params=pltpu.CompilerParams(vmem_limit_bytes=24 << 20),
            name="leave",
        )(hold(ent), hold(acc))
        rel_final = rel.reshape(REL_ROWS, 2, 2 * LANES)[:rel_count, :, :half].reshape(rel_count, emb_dim)
        return table_t.T, state.reshape(rows), rel_final, jnp.stack(losses)[None, :]

    return jax.shard_map(per_device, mesh=mesh, in_specs=(row_spec, state_spec, rel_spec, edge_spec, edge_spec, edge_spec, edge_spec, edge_spec), out_specs=(row_spec, state_spec, rel_spec, row_spec), check_vma=False)
```

```python
import functools

import jax
import jax.numpy as jnp
from jax import lax
from jax.experimental import pallas as pl
from jax.experimental.pallas import tpu as pltpu
from jax.sharding import PartitionSpec as P

LEARN_RATE = 0.25
ADA_EPS = 1e-10
LANES = 128
SUB = 32
CHUNK = 256
REL_ROWS = 256
VMEM = pltpu.VMEM
SMEM = pltpu.SMEM
F32 = jnp.float32
BF16 = jnp.bfloat16


def lane_iota(rows):
    return lax.broadcasted_iota(jnp.int32, (rows, LANES), 1)


def updated(e, a, emb_dim, lane):
    squares = (a[0] * a[0] + a[1] * a[1]) + (a[2] * a[2] + a[3] * a[3])
    state = jnp.sum(squares * (1.0 / emb_dim) + jnp.where(lane == LANES - 1, e[1], 0.0), axis=1, keepdims=True)
    scale = LEARN_RATE * lax.rsqrt(state + ADA_EPS)
    new = [e[c] - scale * a[c] for c in range(4)]
    new[1] = jnp.where(lane == LANES - 1, state, new[1])
    return new


def split3(x):
    hi = x.astype(BF16)
    rest = x - hi.astype(F32)
    mid = rest.astype(BF16)
    return hi, mid, (rest - mid.astype(F32)).astype(BF16)


def write_wire(buf, n, b, x, short, left, lane):
    base = b * SUB
    turned = pltpu.roll(x[3], short, axis=1)
    over = 2 * short - LANES
    rows = lambda part: pl.ds(pl.multiple_of(part * CHUNK + base, SUB), SUB)
    buf[n, rows(0), :] = x[0].astype(BF16)
    buf[n, rows(1), :] = x[2].astype(BF16)
    buf[n, rows(2), :] = jnp.where(lane < short, x[1], turned).astype(BF16)
    return left + pltpu.roll(jnp.where(lane < over, turned, 0.0), b * over, axis=1)


def read_wire(buf, n, b, short, left, lane):
    base = b * SUB
    rows = lambda part: pl.ds(pl.multiple_of(part * CHUNK + base, SUB), SUB)
    over = 2 * short - LANES
    x0 = buf[n, rows(0), :].astype(F32)
    x2 = buf[n, rows(1), :].astype(F32)
    mixed = buf[n, rows(2), :].astype(F32)
    x1 = jnp.where(lane < short, mixed, 0.0)
    kept = LANES - short
    tail = pltpu.roll(left, lax.rem(LANES + kept - b * over, LANES), axis=1)
    x3 = jnp.where(lane < kept, pltpu.roll(mixed, kept, axis=1), jnp.where(lane < short, tail, 0.0))
    return [x0, x1, x2, x3]


def pieces(first, count):
    return [pl.ds(first * 4 + c, count, stride=4) for c in range(4)]


def row_of(r):
    return pl.ds(pl.multiple_of(r * 4, 4), 4)


def cols_of(c):
    return slice(LANES * c, LANES * (c + 1))


def gather_rows(ent, idx, step, start, rows):
    for i in range(SUB):
        r = idx[step, 0, start + i]
        rows[4 * i:4 * i + 4, :] = ent[r]
    return [rows[s, :] for s in pieces(0, SUB)]


def dense_update(ent, acc, first, count, emb_dim):
    lane = lane_iota(SUB)

    def step(j, carry):
        at = pl.multiple_of((first + j) * SUB, SUB)
        here = pieces(at, SUB)
        new = updated([ent[s, :] for s in here], [acc[s, :] for s in here], emb_dim, lane)
        for c in range(4):
            ent[here[c], :] = new[c]
        return carry

    lax.fori_loop(0, count, step, 0, unroll=2)


def merge_repeats(src, at, ids, split, grads, out):
    for p in range(LANES // SUB):
        part = pl.ds(pl.multiple_of(at + p * SUB, SUB), SUB)
        for c in range(4):
            for k, piece in enumerate(split3(src[part, cols_of(c)])):
                split[p * SUB:(p + 1) * SUB, 512 * k + LANES * c:512 * k + LANES * (c + 1)] = piece
    row = jnp.broadcast_to(ids, (LANES, LANES))
    i0 = lax.broadcasted_iota(jnp.int32, (LANES, LANES), 0)
    i1 = lane_iota(LANES)
    same = (jnp.transpose(row) == row) & (i1 <= i0) & (i1 // SUB == i0 // SUB)
    got = jnp.dot(jnp.where(same, 1.0, 0.0).astype(BF16), split[...], preferred_element_type=F32)
    here = pieces(out, LANES)
    for c in range(4):
        grads[here[c], :] = (got[:, cols_of(c)] + got[:, 512 + LANES * c:512 + LANES * (c + 1)]) + got[:, 1024 + LANES * c:1024 + LANES * (c + 1)]


def main_kernel(step, devs, emb_dim, head_idx, tail_idx, neg_idx, head_row, tail_row, neg_row, mask_row, rel_row, loss_in, rel_in, ent,
                grads, rel_out, loss_out,
                rows, rel_split, heads, rels, served, q_send, q_recv, dq_send, dq_recv, q_all, weights, scores,
                pos, d_pos, probs, d_mix, flat, d_head, d_split, m_split, rel_acc, rel_got, rel_half, rel_got1, rel_two, rel_got2, rel_sum,
                loss_send, loss_recv, q_ss, q_rs, d_ss, d_rs, r_ss, r_rs):
    edges = head_idx.shape[2]
    negs = neg_idx.shape[2]
    chunks = edges // CHUNK
    subs = CHUNK // SUB
    half = emb_dim // 2
    short = half - LANES
    score_scale = emb_dim ** -0.5
    shift = step + 1
    me = lax.axis_index("ent")
    owner = lax.rem(me + shift, devs)
    asker = lax.rem(me + devs - shift, devs)
    core = lax.rem(me, 2)
    x_at = lax.rem(me // 2, 2)
    y_at = me // 4
    mate = me + 1 - 2 * core
    x_mate = me + 2 - 4 * x_at
    y_mate = me + 4 - 8 * y_at
    lane = lane_iota(SUB)

    def copy_to(src, dst, send_sem, recv_sem, dev):
        return pltpu.make_async_remote_copy(src_ref=src, dst_ref=dst, send_sem=send_sem, recv_sem=recv_sem,
                                            device_id={"ent": dev}, device_id_type=pl.DeviceIdType.MESH)

    barrier = pltpu.get_barrier_semaphore()
    for dev in (owner, asker, mate, x_mate, y_mate):
        pl.semaphore_signal(barrier, inc=1, device_id={"ent": dev}, device_id_type=pl.DeviceIdType.MESH)
    def split_rel(j, carry):
        at = pl.ds(pl.multiple_of(j * SUB, SUB), SUB)
        for p, part in enumerate(split3(rel_in[at, :])):
            rel_split[at, 512 * p:512 * (p + 1)] = part
        return carry

    lax.fori_loop(0, REL_ROWS // SUB, split_rel, 0)
    def one_hot(n):
        ids = rel_row[step, 0:1, n * CHUNK:(n + 1) * CHUNK]
        return jnp.where(lax.broadcasted_iota(jnp.int32, (REL_ROWS, CHUNK), 0) == ids, 1.0, 0.0).astype(BF16)

    q_copies = []
    for n in range(chunks):
        picked = lax.dot_general(one_hot(n), rel_split[...], (((0,), (0,)), ((), ())), preferred_element_type=F32)
        rels[n * CHUNK:(n + 1) * CHUNK, :] = (picked[:, :512] + picked[:, 512:1024]) + picked[:, 1024:]

        def query(b, left, n=n):
            at = pl.multiple_of(n * CHUNK + b * SUB, SUB)
            h = gather_rows(ent, head_idx, step, at, rows)
            h[1] = jnp.where(lane < short, h[1], 0.0)
            r = [rels[pl.ds(at, SUB), cols_of(c)] for c in range(4)]
            r[1] = jnp.where(lane < short, r[1], 0.0)
            for c in range(4):
                heads[pl.ds(at, SUB), cols_of(c)] = h[c]
            q = [h[0] * r[0] - h[2] * r[2], h[1] * r[1] - h[3] * r[3], h[0] * r[2] + h[2] * r[0], h[1] * r[3] + h[3] * r[1]]
            return write_wire(q_send, n, b, q, short, left, lane)

        left = lax.fori_loop(0, subs, query, jnp.zeros((SUB, LANES), F32))
        q_send[n, 3 * CHUNK:, :] = left.astype(BF16)
        if n == 0:
            pl.semaphore_wait(barrier, 5)
        copy = copy_to(q_send.at[n], q_recv.at[n], q_ss.at[n], q_rs.at[n], owner)
        copy.start()
        q_copies.append(copy)

    def serve(idx, out):
        def one(j, carry):
            at = pl.multiple_of(j * SUB, SUB)
            t = gather_rows(ent, idx, step, at, rows)
            t[1] = jnp.where(lane < short, t[1], 0.0)
            for c in range(4):
                served[pl.ds(pl.multiple_of(out + at, SUB), SUB), cols_of(c)] = t[c].astype(BF16)
            return carry

        lax.fori_loop(0, idx.shape[2] // SUB, one, 0)

    serve(neg_idx, edges)
    serve(tail_idx, 0)

    loss = jnp.zeros((SUB, 1), F32)
    d_copies = []
    for n in range(chunks):
        for p in range(CHUNK // LANES):
            row = mask_row[step, 0:1, n * CHUNK + LANES * p:n * CHUNK + LANES * (p + 1)].astype(F32)
            weights[LANES * p:LANES * (p + 1), :] = jnp.transpose(jnp.broadcast_to(row, (LANES, LANES)))
        q_copies[n].wait_recv()

        def arrive(b, carry, n=n):
            at = pl.multiple_of(b * SUB, SUB)
            q = read_wire(q_recv, n, b, short, q_recv[n, 3 * CHUNK:, :].astype(F32), lane)
            t = [served[pl.ds(pl.multiple_of(n * CHUNK + at, SUB), SUB), cols_of(c)].astype(F32) for c in range(4)]
            pos[pl.ds(at, SUB), :] = score_scale * jnp.sum((q[0] * t[0] + q[1] * t[1]) + (q[2] * t[2] + q[3] * t[3]), axis=1, keepdims=True)
            for c in range(4):
                q_all[pl.ds(at, SUB), cols_of(c)] = q[c].astype(BF16)
            return carry

        lax.fori_loop(0, subs, arrive, 0)
        scores[...] = lax.dot_general(q_all[...], served[edges:, :], (((1,), (1,)), ((), ())), preferred_element_type=F32)

        def soft(b, total):
            at = pl.ds(pl.multiple_of(b * SUB, SUB), SUB)
            s = score_scale * scores[at, :]
            p = pos[at, :]
            w = weights[at, 0:1]
            top = jnp.maximum(p, jnp.max(s, axis=1, keepdims=True))
            e = jnp.exp(s - top)
            pe = jnp.exp(p - top)
            denom = pe + jnp.sum(e, axis=1, keepdims=True)
            d_pos[at, :] = score_scale * (w * (pe / denom - 1.0))
            probs[at, :] = ((w / denom) * e).astype(BF16)
            return total + w * (top + jnp.log(denom) - p)

        loss = lax.fori_loop(0, subs, soft, loss)
        d_mix[...] = jnp.dot(probs[...], served[edges:, :], preferred_element_type=F32)

        def back(b, left, n=n):
            at = pl.multiple_of(b * SUB, SUB)
            dp = d_pos[pl.ds(at, SUB), :]
            row = pl.ds(pl.multiple_of(n * CHUNK + at, SUB), SUB)
            dq = []
            for c in range(4):
                t = served[row, cols_of(c)].astype(F32)
                q = q_all[pl.ds(at, SUB), cols_of(c)].astype(F32)
                dq.append(dp * t + score_scale * d_mix[pl.ds(at, SUB), cols_of(c)])
                flat[row, cols_of(c)] = dp * q
            return write_wire(dq_send, n, b, dq, short, left, lane)

        left = lax.fori_loop(0, subs, back, jnp.zeros((SUB, LANES), F32))
        dq_send[n, 3 * CHUNK:, :] = left.astype(BF16)
        copy = copy_to(dq_send.at[n], dq_recv.at[n], d_ss.at[n], d_rs.at[n], asker)
        copy.start()
        d_copies.append(copy)
        part = lax.dot_general(probs[...], q_all[...], (((0,), (0,)), ((), ())), preferred_element_type=F32)
        if n == 0:
            flat[edges:, :] = part
        elif n < chunks - 1:
            flat[edges:, :] += part
        else:
            flat[edges:, :] = score_scale * (flat[edges:, :] + part)

    loss_send[...] = jnp.broadcast_to(jnp.sum(loss, axis=0, keepdims=True), (8, LANES))
    loss_copy = copy_to(loss_send, loss_recv, r_ss.at[6], r_rs.at[6], asker)
    loss_copy.start()

    def merge(ids, src_at, out):
        def one(j, carry):
            at = pl.multiple_of(j * LANES, LANES)
            merge_repeats(flat, src_at + at, ids[step, 0:1, pl.ds(at, LANES)], m_split, grads, out + at)
            return carry

        lax.fori_loop(0, ids.shape[2] // LANES, one, 0)

    merge(tail_row, 0, edges)
    merge(neg_row, edges, 2 * edges)

    for n in range(chunks):
        d_copies[n].wait_recv()

        def own(b, carry, n=n):
            at = pl.multiple_of(n * CHUNK + b * SUB, SUB)
            dq = read_wire(dq_recv, n, b, short, dq_recv[n, 3 * CHUNK:, :].astype(F32), lane)
            h = [heads[pl.ds(at, SUB), cols_of(c)] for c in range(4)]
            r = [rels[pl.ds(at, SUB), cols_of(c)] for c in range(4)]
            r[1] = jnp.where(lane < short, r[1], 0.0)
            dh = [dq[0] * r[0] + dq[2] * r[2], dq[1] * r[1] + dq[3] * r[3], dq[2] * r[0] - dq[0] * r[2], dq[3] * r[1] - dq[1] * r[3]]
            dr = [dq[0] * h[0] + dq[2] * h[2], dq[1] * h[1] + dq[3] * h[3], dq[2] * h[0] - dq[0] * h[2], dq[3] * h[1] - dq[1] * h[3]]
            row = pl.ds(pl.multiple_of(b * SUB, SUB), SUB)
            for c in range(4):
                d_head[row, cols_of(c)] = dh[c]
                for p, part in enumerate(split3(dr[c])):
                    d_split[row, 512 * p + LANES * c:512 * p + LANES * (c + 1)] = part
            return carry

        lax.fori_loop(0, subs, own, 0)
        part = jnp.dot(one_hot(n), d_split[...], preferred_element_type=F32)
        part = (part[:, :512] + part[:, 512:1024]) + part[:, 1024:]
        if n == 0:
            rel_acc[...] = part
        else:
            rel_acc[...] += part
        if n < chunks - 1:
            for p in range(CHUNK // LANES):
                at = n * CHUNK + p * LANES
                merge_repeats(d_head, p * LANES, head_row[step, 0:1, at:at + LANES], m_split, grads, at)

    hrows = REL_ROWS // 2
    qrows = hrows // 2
    mine = pl.ds(pl.multiple_of(core * hrows, hrows), hrows)
    theirs = pl.ds(pl.multiple_of((1 - core) * hrows, hrows), hrows)
    c0 = copy_to(rel_acc.at[theirs], rel_got, r_ss.at[0], r_rs.at[0], mate)
    c0.start()
    at = (chunks - 1) * CHUNK
    merge_repeats(d_head, 0, head_row[step, 0:1, at:at + LANES], m_split, grads, at)
    c0.wait_recv()
    rel_half[...] = (rel_acc[mine, :] + rel_got[...]).astype(BF16)
    first, last = pl.ds(0, qrows), pl.ds(qrows, qrows)
    c1 = copy_to(rel_half.at[first], rel_got1.at[first], r_ss.at[1], r_rs.at[1], x_mate)
    c2 = copy_to(rel_half.at[last], rel_got1.at[last], r_ss.at[2], r_rs.at[2], y_mate)
    c1.start()
    c2.start()
    for p in range(1, CHUNK // LANES):
        at = (chunks - 1) * CHUNK + p * LANES
        merge_repeats(d_head, p * LANES, head_row[step, 0:1, at:at + LANES], m_split, grads, at)
    c1.wait_recv()
    rel_two[first, :] = (rel_half[first, :].astype(F32) + rel_got1[first, :].astype(F32)).astype(BF16)
    c3 = copy_to(rel_two.at[first], rel_got2.at[first], r_ss.at[3], r_rs.at[3], y_mate)
    c3.start()
    c2.wait_recv()
    rel_two[last, :] = (rel_half[last, :].astype(F32) + rel_got1[last, :].astype(F32)).astype(BF16)
    c4 = copy_to(rel_two.at[last], rel_got2.at[last], r_ss.at[4], r_rs.at[4], x_mate)
    c4.start()
    c3.wait_recv()
    c4.wait_recv()
    rel_sum[mine, :] = rel_two[...].astype(F32) + rel_got2[...].astype(F32)
    c5 = copy_to(rel_sum.at[mine], rel_sum.at[mine], r_ss.at[5], r_rs.at[5], mate)
    c5.start()
    loss_copy.wait_recv()
    loss_out[...] = loss_in[...] + jnp.where(lane_iota(8) == step, loss_recv[...] * (1.0 / edges), 0.0)
    c5.wait_recv()

    def rel_step(j, carry):
        at = pl.ds(pl.multiple_of(j * SUB, SUB), SUB)
        new = updated([rel_in[at, cols_of(c)] for c in range(4)], [rel_sum[at, cols_of(c)] for c in range(4)], emb_dim, lane)
        for c in range(4):
            rel_out[at, cols_of(c)] = new[c]
        return carry

    lax.fori_loop(0, REL_ROWS // SUB, rel_step, 0)
    for copy in q_copies + d_copies + [loss_copy, c0, c1, c2, c3, c4, c5]:
        copy.wait_send()


def scatter_kernel(step, emb_dim, head_hbm, tail_hbm, neg_hbm, grads, ent_in, ent, acc, head_idx, tail_idx, neg_idx, sems):
    lists = ((head_hbm, head_idx), (tail_hbm, tail_idx), (neg_hbm, neg_idx))
    fetches = [pltpu.make_async_copy(src.at[step], dst, sems.at[k]) for k, (src, dst) in enumerate(lists)]
    for fetch in fetches:
        fetch.start()

    def clear(j, carry):
        acc[pl.ds(pl.multiple_of(j * 512, 512), 512), :] = jnp.zeros((512, LANES), F32)
        return carry

    lax.fori_loop(0, acc.shape[0] // 512, clear, 0)
    base = 0
    for fetch, (_, idx) in zip(fetches, lists):
        fetch.wait()

        def block(j, carry, idx=idx, base=base):
            at = j * SUB
            rows = [row_of(idx[0, at + i]) for i in range(SUB)]
            new = [acc[rows[i], :] + grads[row_of(base + at + i), :] for i in range(SUB)]
            for i in range(SUB):
                acc[rows[i], :] = new[i]
            return carry

        lax.fori_loop(0, idx.shape[1] // SUB, block, 0)
        base += idx.shape[1]
    dense_update(ent, acc, 0, ent.shape[0] // (4 * SUB), emb_dim)


def swap_kernel(devs, tail, neg, mask, tail_got, neg_got, mask_got, ss, rs):
    me = lax.axis_index("ent")
    barrier = pltpu.get_barrier_semaphore()
    for d in range(1, devs):
        pl.semaphore_signal(barrier, inc=1, device_id={"ent": lax.rem(me + d, devs)}, device_id_type=pl.DeviceIdType.MESH)
    pl.semaphore_wait(barrier, devs - 1)
    copies = []
    for s in range(tail.shape[0]):
        owner = lax.rem(me + s + 1, devs)
        for k, (src, dst) in enumerate(((tail, tail_got), (neg, neg_got), (mask, mask_got))):
            copies.append(pltpu.make_async_remote_copy(src_ref=src.at[s], dst_ref=dst.at[s], send_sem=ss.at[s, k], recv_sem=rs.at[s, k],
                                                       device_id={"ent": owner}, device_id_type=pl.DeviceIdType.MESH))
            copies[-1].start()
    for copy in copies:
        copy.wait()


def enter_kernel(table, state, rel, ent, rel_out, loss_out, pad):
    blk = pl.program_id(0)
    cols = table.shape[1]
    half = table.shape[0] // 2
    short = half - LANES

    def piece(src, c, lanes, extra=None):
        first = (c // 2) * half
        width = lanes.stop - lanes.start
        if c % 2 == 0 and width == LANES:
            return src[first:first + LANES, lanes]
        count = LANES if c % 2 == 0 else short
        pad[...] = jnp.zeros((LANES, LANES), F32)
        pad[0:count, 0:width] = src[first + LANES * (c % 2):first + LANES * (c % 2) + count, lanes]
        if extra is not None:
            pad[LANES - 1:LANES, :] = extra
        return pad[...]

    @pl.when(blk == 0)
    def _():
        loss_out[...] = jnp.zeros_like(loss_out)
        count = rel.shape[1]
        for p in range(REL_ROWS // LANES):
            for c in range(4):
                rel_out[LANES * p:LANES * (p + 1), cols_of(c)] = jnp.transpose(piece(rel, c, slice(LANES * p, min(LANES * (p + 1), count))))

    for j in range(cols // LANES):
        lanes = slice(LANES * j, LANES * (j + 1))
        here = pieces(pl.multiple_of(blk * cols + j * LANES, LANES), LANES)
        for c in range(4):
            ent[here[c], :] = jnp.transpose(piece(table, c, lanes, state[j:j + 1, :] if c == 1 else None))


def leave_kernel(emb_dim, ent, rel, loss, table, state, rel_out, loss_out):
    blk = pl.program_id(0)
    cols = table.shape[1]
    half = emb_dim // 2
    short = half - LANES
    count = rel_out.shape[1]

    def put(dst, c, lanes, x):
        first = (c // 2) * half + LANES * (c % 2)
        rows = short if c % 2 else LANES
        dst[first:first + rows, lanes] = x[0:rows, 0:lanes.stop - lanes.start]

    @pl.when(blk == 0)
    def _():
        loss_out[...] = loss[...]
        for p in range(REL_ROWS // LANES):
            for c in range(4):
                put(rel_out, c, slice(LANES * p, min(LANES * (p + 1), count)), jnp.transpose(rel[LANES * p:LANES * (p + 1), cols_of(c)]))

    for j in range(cols // LANES):
        at = pl.multiple_of(blk * cols + j * LANES, LANES)
        lanes = slice(LANES * j, LANES * (j + 1))
        here = pieces(at, LANES)
        for c in range(4):
            turned = jnp.transpose(ent[here[c], :])
            put(table, c, lanes, turned)
            if c == 1:
                state[j:j + 1, :] = turned[LANES - 1:LANES, :]


def solution(mesh):
    devs = mesh.shape["ent"]
    row_spec = P(("sweep", "ent"), None)
    state_spec = P(("sweep", "ent"))
    rel_spec = P("sweep", None)
    edge_spec = P(("sweep", "ent"), None, None)
    in_vmem = pl.BlockSpec(memory_space=VMEM)
    in_smem = pl.BlockSpec(memory_space=SMEM)
    in_any = pl.BlockSpec(memory_space=pl.ANY)
    hold = lambda x: pltpu.with_memory_space_constraint(x, VMEM)
    DMA = pltpu.SemaphoreType.DMA

    def per_device(ent_part, ada_part, rel_table, head_idx, tail_idx, rel_idx, neg_idx, edge_mask):
        rows, emb_dim = ent_part.shape
        rounds, edges = head_idx.shape[1:]
        negs = neg_idx.shape[2]
        chunks = edges // CHUNK
        total = 2 * edges + negs
        table_vmem = VMEM((rows * 4, LANES), F32)
        rel_vmem = VMEM((REL_ROWS, 4 * LANES), F32)
        loss_vmem = VMEM((8, LANES), F32)
        block = min(1024, rows)
        by_round = lambda x: x.transpose(1, 0, 2)
        head_idx, tail_idx, rel_idx, neg_idx, edge_mask = map(by_round, (head_idx, tail_idx, rel_idx, neg_idx, edge_mask))
        table_spec = pl.BlockSpec((emb_dim, block), lambda i: (0, i))
        ada_spec = pl.BlockSpec((block // LANES, LANES), lambda i: (i, 0))

        tail_got, neg_got, mask_got = pl.pallas_call(
            functools.partial(swap_kernel, devs),
            out_shape=tuple(jax.ShapeDtypeStruct(x.shape, x.dtype) for x in (tail_idx, neg_idx, edge_mask)),
            in_specs=[in_any] * 3,
            out_specs=(in_any,) * 3,
            scratch_shapes=[DMA((rounds, 3)), DMA((rounds, 3))],
            compiler_params=pltpu.CompilerParams(collective_id=rounds, has_side_effects=True, vmem_limit_bytes=1 << 20),
            name="swap",
        )(tail_idx, neg_idx, edge_mask)
        ent, rel, loss = pl.pallas_call(
            enter_kernel,
            grid=(rows // block,),
            out_shape=(table_vmem, rel_vmem, loss_vmem),
            in_specs=[table_spec, ada_spec, in_vmem],
            out_specs=(in_vmem,) * 3,
            scratch_shapes=[VMEM((LANES, LANES), F32)],
            compiler_params=pltpu.CompilerParams(vmem_limit_bytes=25 << 20),
            name="enter",
        )(ent_part.T, ada_part.reshape(rows // LANES, LANES), rel_table.T)

        wire = VMEM((chunks, 3 * CHUNK + SUB, LANES), BF16)
        full = VMEM((edges, 4 * LANES), F32)
        some = VMEM((CHUNK, 4 * LANES), F32)
        half_rel = (REL_ROWS // 2, 4 * LANES)
        lists = [SMEM((1, edges), jnp.int32), SMEM((1, edges), jnp.int32), SMEM((1, negs), jnp.int32)]
        for step in range(rounds):
            grads, rel, loss = pl.pallas_call(
                functools.partial(main_kernel, step, devs, emb_dim),
                out_shape=(VMEM((total * 4, LANES), F32), rel_vmem, loss_vmem),
                in_specs=[in_smem] * 3 + [in_vmem] * 8,
                out_specs=(in_vmem,) * 3,
                scratch_shapes=[
                    VMEM((4 * SUB, LANES), F32), VMEM((REL_ROWS, 12 * LANES), BF16), full, full,
                    VMEM((edges + negs, 4 * LANES), BF16), wire, wire, wire, wire,
                    VMEM((CHUNK, 4 * LANES), BF16), VMEM((CHUNK, LANES), F32), VMEM((CHUNK, negs), F32),
                    VMEM((CHUNK, 1), F32), VMEM((CHUNK, 1), F32), VMEM((CHUNK, negs), BF16), some,
                    VMEM((edges + negs, 4 * LANES), F32), some, VMEM((CHUNK, 12 * LANES), BF16), VMEM((LANES, 12 * LANES), BF16),
                    VMEM((REL_ROWS, 4 * LANES), F32), VMEM(half_rel, F32), VMEM(half_rel, BF16), VMEM(half_rel, BF16), VMEM(half_rel, BF16), VMEM(half_rel, BF16),
                    VMEM((REL_ROWS, 4 * LANES), F32), VMEM((8, LANES), F32), VMEM((8, LANES), F32),
                ] + [DMA((chunks,))] * 4 + [DMA((7,))] * 2,
                compiler_params=pltpu.CompilerParams(collective_id=step, has_side_effects=True, vmem_limit_bytes=25 << 20),
                name="train",
            )(head_idx, tail_got, neg_got, head_idx, tail_got, neg_got, mask_got, rel_idx, hold(loss), hold(rel), hold(ent.reshape(rows, 4, LANES)))
            ent = pl.pallas_call(
                functools.partial(scatter_kernel, step, emb_dim),
                out_shape=table_vmem,
                in_specs=[in_any] * 3 + [in_vmem] * 2,
                out_specs=in_vmem,
                input_output_aliases={4: 0},
                scratch_shapes=[VMEM((rows * 4, LANES), F32)] + lists + [DMA((3,))],
                compiler_params=pltpu.CompilerParams(vmem_limit_bytes=18 << 20),
                name="scatter",
            )(head_idx, tail_got, neg_got, hold(grads), hold(ent))

        table_t, state, rel_t, loss = pl.pallas_call(
            functools.partial(leave_kernel, emb_dim),
            grid=(rows // block,),
            out_shape=(jax.ShapeDtypeStruct((emb_dim, rows), F32), jax.ShapeDtypeStruct((rows // LANES, LANES), F32),
                       jax.ShapeDtypeStruct(rel_table.T.shape, F32), jax.ShapeDtypeStruct((8, LANES), F32)),
            in_specs=[in_vmem] * 3,
            out_specs=(table_spec, ada_spec, in_vmem, in_vmem),
            compiler_params=pltpu.CompilerParams(vmem_limit_bytes=25 << 20),
            name="leave",
        )(hold(ent), hold(rel), hold(loss))
        return table_t.T, state.reshape(rows), rel_t.T, loss[0:1, 0:rounds]

    return jax.shard_map(per_device, mesh=mesh, in_specs=(row_spec, state_spec, rel_spec, edge_spec, edge_spec, edge_spec, edge_spec, edge_spec), out_specs=(row_spec, state_spec, rel_spec, row_spec), check_vma=False)
```

```python
import functools

import jax
import jax.numpy as jnp
from jax import lax
from jax.experimental import pallas as pl
from jax.experimental.pallas import tpu as pltpu
from jax.sharding import PartitionSpec as P

LEARN_RATE = 0.25
ADA_EPS = 1e-10
LANES = 128
SUB = 32
CHUNK = 256
REL_ROWS = 256
VMEM = pltpu.VMEM
SMEM = pltpu.SMEM
F32 = jnp.float32
BF16 = jnp.bfloat16


def lane_iota(rows):
    return lax.broadcasted_iota(jnp.int32, (rows, LANES), 1)


def updated(e, a, emb_dim, lane):
    squares = (a[0] * a[0] + a[1] * a[1]) + (a[2] * a[2] + a[3] * a[3])
    state = jnp.sum(squares * (1.0 / emb_dim) + jnp.where(lane == LANES - 1, e[1], 0.0), axis=1, keepdims=True)
    scale = LEARN_RATE * lax.rsqrt(state + ADA_EPS)
    new = [e[c] - scale * a[c] for c in range(4)]
    new[1] = jnp.where(lane == LANES - 1, state, new[1])
    return new


def split3(x):
    hi = x.astype(BF16)
    rest = x - hi.astype(F32)
    mid = rest.astype(BF16)
    return hi, mid, (rest - mid.astype(F32)).astype(BF16)


def write_wire(buf, n, b, x, short, left, lane):
    base = b * SUB
    turned = pltpu.roll(x[3], short, axis=1)
    over = 2 * short - LANES
    rows = lambda part: pl.ds(pl.multiple_of(part * CHUNK + base, SUB), SUB)
    buf[n, rows(0), :] = x[0].astype(BF16)
    buf[n, rows(1), :] = x[2].astype(BF16)
    buf[n, rows(2), :] = jnp.where(lane < short, x[1], turned).astype(BF16)
    return left + pltpu.roll(jnp.where(lane < over, turned, 0.0), b * over, axis=1)


def read_wire(buf, n, b, short, left, lane):
    base = b * SUB
    rows = lambda part: pl.ds(pl.multiple_of(part * CHUNK + base, SUB), SUB)
    over = 2 * short - LANES
    x0 = buf[n, rows(0), :].astype(F32)
    x2 = buf[n, rows(1), :].astype(F32)
    mixed = buf[n, rows(2), :].astype(F32)
    x1 = jnp.where(lane < short, mixed, 0.0)
    kept = LANES - short
    tail = pltpu.roll(left, lax.rem(LANES + kept - b * over, LANES), axis=1)
    x3 = jnp.where(lane < kept, pltpu.roll(mixed, kept, axis=1), jnp.where(lane < short, tail, 0.0))
    return [x0, x1, x2, x3]


def pieces(first, count):
    return [pl.ds(first * 4 + c, count, stride=4) for c in range(4)]


def row_of(r):
    return pl.ds(pl.multiple_of(r * 4, 4), 4)


def cols_of(c):
    return slice(LANES * c, LANES * (c + 1))


def gather_rows(ent, idx, step, start, rows):
    for i in range(SUB):
        r = idx[step, 0, start + i]
        rows[4 * i:4 * i + 4, :] = ent[r]
    return [rows[s, :] for s in pieces(0, SUB)]


def dense_update(ent, acc, states, emb_dim):
    lane = lane_iota(SUB)
    rows = states.shape[0]

    def block(o, carry):
        def measure(j, c):
            here = pieces(pl.multiple_of(o * rows + j * SUB, SUB), SUB)
            a = [acc[s, :] for s in here]
            squares = (a[0] * a[0] + a[1] * a[1]) + (a[2] * a[2] + a[3] * a[3])
            state = jnp.sum(squares * (1.0 / emb_dim) + jnp.where(lane == LANES - 1, ent[here[1], :], 0.0), axis=1, keepdims=True)
            states[pl.ds(pl.multiple_of(j * SUB, SUB), SUB), :] = jnp.broadcast_to(state, (SUB, LANES))
            return c

        def apply(j, c):
            here = pieces(pl.multiple_of(o * rows + j * SUB, SUB), SUB)
            state = states[pl.ds(pl.multiple_of(j * SUB, SUB), SUB), :]
            scale = LEARN_RATE * lax.rsqrt(state + ADA_EPS)
            for k in range(4):
                new = ent[here[k], :] - scale * acc[here[k], :]
                ent[here[k], :] = jnp.where(lane == LANES - 1, state, new) if k == 1 else new
            return c

        lax.fori_loop(0, rows // SUB, measure, 0, unroll=8)
        lax.fori_loop(0, rows // SUB, apply, 0, unroll=4)
        return carry

    lax.fori_loop(0, ent.shape[0] // (4 * rows), block, 0)


def merge_repeats(src, at, ids, split, grads, out):
    for p in range(LANES // SUB):
        part = pl.ds(pl.multiple_of(at + p * SUB, SUB), SUB)
        for c in range(4):
            for k, piece in enumerate(split3(src[part, cols_of(c)])):
                split[p * SUB:(p + 1) * SUB, 512 * k + LANES * c:512 * k + LANES * (c + 1)] = piece
    row = jnp.broadcast_to(ids, (LANES, LANES))
    i0 = lax.broadcasted_iota(jnp.int32, (LANES, LANES), 0)
    i1 = lane_iota(LANES)
    same = (jnp.transpose(row) == row) & (i1 <= i0) & (i1 // SUB == i0 // SUB)
    got = jnp.dot(jnp.where(same, 1.0, 0.0).astype(BF16), split[...], preferred_element_type=F32)
    here = pieces(out, LANES)
    for c in range(4):
        grads[here[c], :] = (got[:, cols_of(c)] + got[:, 512 + LANES * c:512 + LANES * (c + 1)]) + got[:, 1024 + LANES * c:1024 + LANES * (c + 1)]


def main_kernel(step, devs, emb_dim, head_idx, tail_idx, neg_idx, head_row, tail_row, neg_row, mask_row, rel_row, loss_in, rel_in, ent,
                grads, rel_out, loss_out,
                rows, rel_split, heads, rels, served, q_send, q_recv, dq_send, dq_recv, q_all, weights, scores,
                pos, d_pos, probs, d_mix, flat, d_head, d_split, m_split, rel_acc, rel_got, rel_half, rel_got1, rel_two, rel_got2, rel_sum,
                loss_send, loss_recv, q_ss, q_rs, d_ss, d_rs, r_ss, r_rs):
    edges = head_idx.shape[2]
    negs = neg_idx.shape[2]
    chunks = edges // CHUNK
    subs = CHUNK // SUB
    half = emb_dim // 2
    short = half - LANES
    score_scale = emb_dim ** -0.5
    shift = step + 1
    me = lax.axis_index("ent")
    owner = lax.rem(me + shift, devs)
    asker = lax.rem(me + devs - shift, devs)
    core = lax.rem(me, 2)
    x_at = lax.rem(me // 2, 2)
    y_at = me // 4
    mate = me + 1 - 2 * core
    x_mate = me + 2 - 4 * x_at
    y_mate = me + 4 - 8 * y_at
    lane = lane_iota(SUB)

    def copy_to(src, dst, send_sem, recv_sem, dev):
        return pltpu.make_async_remote_copy(src_ref=src, dst_ref=dst, send_sem=send_sem, recv_sem=recv_sem,
                                            device_id={"ent": dev}, device_id_type=pl.DeviceIdType.MESH)

    barrier = pltpu.get_barrier_semaphore()
    for dev in (owner, asker, mate, x_mate, y_mate):
        pl.semaphore_signal(barrier, inc=1, device_id={"ent": dev}, device_id_type=pl.DeviceIdType.MESH)
    def split_rel(j, carry):
        at = pl.ds(pl.multiple_of(j * SUB, SUB), SUB)
        for p, part in enumerate(split3(rel_in[at, :])):
            rel_split[at, 512 * p:512 * (p + 1)] = part
        return carry

    lax.fori_loop(0, REL_ROWS // SUB, split_rel, 0)
    def one_hot(n):
        ids = rel_row[step, 0:1, n * CHUNK:(n + 1) * CHUNK]
        return jnp.where(lax.broadcasted_iota(jnp.int32, (REL_ROWS, CHUNK), 0) == ids, 1.0, 0.0).astype(BF16)

    q_copies = []
    for n in range(chunks):
        picked = lax.dot_general(one_hot(n), rel_split[...], (((0,), (0,)), ((), ())), preferred_element_type=F32)
        rels[n * CHUNK:(n + 1) * CHUNK, :] = (picked[:, :512] + picked[:, 512:1024]) + picked[:, 1024:]

        def query(b, left, n=n):
            at = pl.multiple_of(n * CHUNK + b * SUB, SUB)
            h = gather_rows(ent, head_idx, step, at, rows)
            h[1] = jnp.where(lane < short, h[1], 0.0)
            r = [rels[pl.ds(at, SUB), cols_of(c)] for c in range(4)]
            r[1] = jnp.where(lane < short, r[1], 0.0)
            for c in range(4):
                heads[pl.ds(at, SUB), cols_of(c)] = h[c]
            q = [h[0] * r[0] - h[2] * r[2], h[1] * r[1] - h[3] * r[3], h[0] * r[2] + h[2] * r[0], h[1] * r[3] + h[3] * r[1]]
            return write_wire(q_send, n, b, q, short, left, lane)

        left = lax.fori_loop(0, subs, query, jnp.zeros((SUB, LANES), F32), unroll=4)
        q_send[n, 3 * CHUNK:, :] = left.astype(BF16)
        if n == 0:
            pl.semaphore_wait(barrier, 5)
        copy = copy_to(q_send.at[n], q_recv.at[n], q_ss.at[n], q_rs.at[n], owner)
        copy.start()
        q_copies.append(copy)

    def serve(idx, out):
        def one(j, carry):
            at = pl.multiple_of(j * SUB, SUB)
            t = gather_rows(ent, idx, step, at, rows)
            t[1] = jnp.where(lane < short, t[1], 0.0)
            for c in range(4):
                served[pl.ds(pl.multiple_of(out + at, SUB), SUB), cols_of(c)] = t[c].astype(BF16)
            return carry

        lax.fori_loop(0, idx.shape[2] // SUB, one, 0, unroll=4)

    serve(neg_idx, edges)
    serve(tail_idx, 0)

    loss = jnp.zeros((SUB, 1), F32)
    d_copies = []
    for n in range(chunks):
        for p in range(CHUNK // LANES):
            row = mask_row[step, 0:1, n * CHUNK + LANES * p:n * CHUNK + LANES * (p + 1)].astype(F32)
            weights[LANES * p:LANES * (p + 1), :] = jnp.transpose(jnp.broadcast_to(row, (LANES, LANES)))
        q_copies[n].wait_recv()

        def arrive(b, carry, n=n):
            at = pl.multiple_of(b * SUB, SUB)
            q = read_wire(q_recv, n, b, short, q_recv[n, 3 * CHUNK:, :].astype(F32), lane)
            t = [served[pl.ds(pl.multiple_of(n * CHUNK + at, SUB), SUB), cols_of(c)].astype(F32) for c in range(4)]
            pos[pl.ds(at, SUB), :] = score_scale * jnp.sum((q[0] * t[0] + q[1] * t[1]) + (q[2] * t[2] + q[3] * t[3]), axis=1, keepdims=True)
            for c in range(4):
                q_all[pl.ds(at, SUB), cols_of(c)] = q[c].astype(BF16)
            return carry

        lax.fori_loop(0, subs, arrive, 0, unroll=4)
        scores[...] = lax.dot_general(q_all[...], served[edges:, :], (((1,), (1,)), ((), ())), preferred_element_type=F32)

        def soft(b, total):
            at = pl.ds(pl.multiple_of(b * SUB, SUB), SUB)
            s = score_scale * scores[at, :]
            p = pos[at, :]
            w = weights[at, 0:1]
            top = jnp.maximum(p, jnp.max(s, axis=1, keepdims=True))
            e = jnp.exp(s - top)
            pe = jnp.exp(p - top)
            denom = pe + jnp.sum(e, axis=1, keepdims=True)
            d_pos[at, :] = score_scale * (w * (pe / denom - 1.0))
            probs[at, :] = ((w / denom) * e).astype(BF16)
            return total + w * (top + jnp.log(denom) - p)

        loss = lax.fori_loop(0, subs, soft, loss, unroll=4)
        d_mix[...] = jnp.dot(probs[...], served[edges:, :], preferred_element_type=F32)

        def back(b, left, n=n):
            at = pl.multiple_of(b * SUB, SUB)
            dp = d_pos[pl.ds(at, SUB), :]
            row = pl.ds(pl.multiple_of(n * CHUNK + at, SUB), SUB)
            dq = []
            for c in range(4):
                t = served[row, cols_of(c)].astype(F32)
                q = q_all[pl.ds(at, SUB), cols_of(c)].astype(F32)
                dq.append(dp * t + score_scale * d_mix[pl.ds(at, SUB), cols_of(c)])
                flat[row, cols_of(c)] = dp * q
            return write_wire(dq_send, n, b, dq, short, left, lane)

        left = lax.fori_loop(0, subs, back, jnp.zeros((SUB, LANES), F32), unroll=4)
        dq_send[n, 3 * CHUNK:, :] = left.astype(BF16)
        copy = copy_to(dq_send.at[n], dq_recv.at[n], d_ss.at[n], d_rs.at[n], asker)
        copy.start()
        d_copies.append(copy)
        part = lax.dot_general(probs[...], q_all[...], (((0,), (0,)), ((), ())), preferred_element_type=F32)
        if n == 0:
            flat[edges:, :] = part
        elif n < chunks - 1:
            flat[edges:, :] += part
        else:
            flat[edges:, :] = score_scale * (flat[edges:, :] + part)

    loss_send[...] = jnp.broadcast_to(jnp.sum(loss, axis=0, keepdims=True), (8, LANES))
    loss_copy = copy_to(loss_send, loss_recv, r_ss.at[6], r_rs.at[6], asker)
    loss_copy.start()

    def merge(ids, src_at, out):
        def one(j, carry):
            at = pl.multiple_of(j * LANES, LANES)
            merge_repeats(flat, src_at + at, ids[step, 0:1, pl.ds(at, LANES)], m_split, grads, out + at)
            return carry

        lax.fori_loop(0, ids.shape[2] // LANES, one, 0, unroll=2)

    merge(tail_row, 0, edges)
    merge(neg_row, edges, 2 * edges)

    for n in range(chunks):
        d_copies[n].wait_recv()

        def own(b, carry, n=n):
            at = pl.multiple_of(n * CHUNK + b * SUB, SUB)
            dq = read_wire(dq_recv, n, b, short, dq_recv[n, 3 * CHUNK:, :].astype(F32), lane)
            h = [heads[pl.ds(at, SUB), cols_of(c)] for c in range(4)]
            r = [rels[pl.ds(at, SUB), cols_of(c)] for c in range(4)]
            r[1] = jnp.where(lane < short, r[1], 0.0)
            dh = [dq[0] * r[0] + dq[2] * r[2], dq[1] * r[1] + dq[3] * r[3], dq[2] * r[0] - dq[0] * r[2], dq[3] * r[1] - dq[1] * r[3]]
            dr = [dq[0] * h[0] + dq[2] * h[2], dq[1] * h[1] + dq[3] * h[3], dq[2] * h[0] - dq[0] * h[2], dq[3] * h[1] - dq[1] * h[3]]
            row = pl.ds(pl.multiple_of(b * SUB, SUB), SUB)
            for c in range(4):
                d_head[row, cols_of(c)] = dh[c]
                for p, part in enumerate(split3(dr[c])):
                    d_split[row, 512 * p + LANES * c:512 * p + LANES * (c + 1)] = part
            return carry

        lax.fori_loop(0, subs, own, 0, unroll=4)
        part = jnp.dot(one_hot(n), d_split[...], preferred_element_type=F32)
        part = (part[:, :512] + part[:, 512:1024]) + part[:, 1024:]
        if n == 0:
            rel_acc[...] = part
        else:
            rel_acc[...] += part
        if n < chunks - 1:
            for p in range(CHUNK // LANES):
                at = n * CHUNK + p * LANES
                merge_repeats(d_head, p * LANES, head_row[step, 0:1, at:at + LANES], m_split, grads, at)

    hrows = REL_ROWS // 2
    qrows = hrows // 2
    mine = pl.ds(pl.multiple_of(core * hrows, hrows), hrows)
    theirs = pl.ds(pl.multiple_of((1 - core) * hrows, hrows), hrows)
    c0 = copy_to(rel_acc.at[theirs], rel_got, r_ss.at[0], r_rs.at[0], mate)
    c0.start()
    at = (chunks - 1) * CHUNK
    merge_repeats(d_head, 0, head_row[step, 0:1, at:at + LANES], m_split, grads, at)
    c0.wait_recv()
    rel_half[...] = (rel_acc[mine, :] + rel_got[...]).astype(BF16)
    first, last = pl.ds(0, qrows), pl.ds(qrows, qrows)
    c1 = copy_to(rel_half.at[first], rel_got1.at[first], r_ss.at[1], r_rs.at[1], x_mate)
    c2 = copy_to(rel_half.at[last], rel_got1.at[last], r_ss.at[2], r_rs.at[2], y_mate)
    c1.start()
    c2.start()
    for p in range(1, CHUNK // LANES):
        at = (chunks - 1) * CHUNK + p * LANES
        merge_repeats(d_head, p * LANES, head_row[step, 0:1, at:at + LANES], m_split, grads, at)
    c1.wait_recv()
    rel_two[first, :] = (rel_half[first, :].astype(F32) + rel_got1[first, :].astype(F32)).astype(BF16)
    c3 = copy_to(rel_two.at[first], rel_got2.at[first], r_ss.at[3], r_rs.at[3], y_mate)
    c3.start()
    c2.wait_recv()
    rel_two[last, :] = (rel_half[last, :].astype(F32) + rel_got1[last, :].astype(F32)).astype(BF16)
    c4 = copy_to(rel_two.at[last], rel_got2.at[last], r_ss.at[4], r_rs.at[4], x_mate)
    c4.start()
    c3.wait_recv()
    c4.wait_recv()
    rel_sum[mine, :] = rel_two[...].astype(F32) + rel_got2[...].astype(F32)
    c5 = copy_to(rel_sum.at[mine], rel_sum.at[mine], r_ss.at[5], r_rs.at[5], mate)
    c5.start()
    loss_copy.wait_recv()
    loss_out[...] = loss_in[...] + jnp.where(lane_iota(8) == step, loss_recv[...] * (1.0 / edges), 0.0)
    c5.wait_recv()

    def rel_step(j, carry):
        at = pl.ds(pl.multiple_of(j * SUB, SUB), SUB)
        new = updated([rel_in[at, cols_of(c)] for c in range(4)], [rel_sum[at, cols_of(c)] for c in range(4)], emb_dim, lane)
        for c in range(4):
            rel_out[at, cols_of(c)] = new[c]
        return carry

    lax.fori_loop(0, REL_ROWS // SUB, rel_step, 0, unroll=4)
    for copy in q_copies + d_copies + [loss_copy, c0, c1, c2, c3, c4, c5]:
        copy.wait_send()


def scatter_kernel(step, emb_dim, head_hbm, tail_hbm, neg_hbm, grads, ent_in, ent, acc, states, head_idx, tail_idx, neg_idx, sems):
    lists = ((head_hbm, head_idx), (tail_hbm, tail_idx), (neg_hbm, neg_idx))
    fetches = [pltpu.make_async_copy(src.at[step], dst, sems.at[k]) for k, (src, dst) in enumerate(lists)]
    for fetch in fetches:
        fetch.start()

    def clear(j, carry):
        acc[pl.ds(pl.multiple_of(j * 512, 512), 512), :] = jnp.zeros((512, LANES), F32)
        return carry

    lax.fori_loop(0, acc.shape[0] // 512, clear, 0)
    base = 0
    for fetch, (_, idx) in zip(fetches, lists):
        fetch.wait()

        def block(j, carry, idx=idx, base=base):
            at = j * SUB
            rows = [row_of(idx[0, at + i]) for i in range(SUB)]
            new = [acc[rows[i], :] + grads[row_of(base + at + i), :] for i in range(SUB)]
            for i in range(SUB):
                acc[rows[i], :] = new[i]
            return carry

        lax.fori_loop(0, idx.shape[1] // SUB, block, 0)
        base += idx.shape[1]
    dense_update(ent, acc, states, emb_dim)


def swap_kernel(devs, tail, neg, mask, tail_got, neg_got, mask_got, ss, rs):
    me = lax.axis_index("ent")
    barrier = pltpu.get_barrier_semaphore()
    for d in range(1, devs):
        pl.semaphore_signal(barrier, inc=1, device_id={"ent": lax.rem(me + d, devs)}, device_id_type=pl.DeviceIdType.MESH)
    pl.semaphore_wait(barrier, devs - 1)
    copies = []
    for s in range(tail.shape[0]):
        owner = lax.rem(me + s + 1, devs)
        for k, (src, dst) in enumerate(((tail, tail_got), (neg, neg_got), (mask, mask_got))):
            copies.append(pltpu.make_async_remote_copy(src_ref=src.at[s], dst_ref=dst.at[s], send_sem=ss.at[s, k], recv_sem=rs.at[s, k],
                                                       device_id={"ent": owner}, device_id_type=pl.DeviceIdType.MESH))
            copies[-1].start()
    for copy in copies:
        copy.wait()


def enter_kernel(table, state, rel, ent, rel_out, loss_out, pad):
    blk = pl.program_id(0)
    cols = table.shape[1]
    half = table.shape[0] // 2
    short = half - LANES

    def piece(src, c, lanes, extra=None):
        first = (c // 2) * half
        width = lanes.stop - lanes.start
        if c % 2 == 0 and width == LANES:
            return src[first:first + LANES, lanes]
        count = LANES if c % 2 == 0 else short
        pad[...] = jnp.zeros((LANES, LANES), F32)
        pad[0:count, 0:width] = src[first + LANES * (c % 2):first + LANES * (c % 2) + count, lanes]
        if extra is not None:
            pad[LANES - 1:LANES, :] = extra
        return pad[...]

    @pl.when(blk == 0)
    def _():
        loss_out[...] = jnp.zeros_like(loss_out)
        count = rel.shape[1]
        for p in range(REL_ROWS // LANES):
            for c in range(4):
                rel_out[LANES * p:LANES * (p + 1), cols_of(c)] = jnp.transpose(piece(rel, c, slice(LANES * p, min(LANES * (p + 1), count))))

    for j in range(cols // LANES):
        lanes = slice(LANES * j, LANES * (j + 1))
        here = pieces(pl.multiple_of(blk * cols + j * LANES, LANES), LANES)
        for c in range(4):
            ent[here[c], :] = jnp.transpose(piece(table, c, lanes, state[j:j + 1, :] if c == 1 else None))


def leave_kernel(emb_dim, ent, rel, loss, table, state, rel_out, loss_out):
    blk = pl.program_id(0)
    cols = table.shape[1]
    half = emb_dim // 2
    short = half - LANES
    count = rel_out.shape[1]

    def put(dst, c, lanes, x):
        first = (c // 2) * half + LANES * (c % 2)
        rows = short if c % 2 else LANES
        dst[first:first + rows, lanes] = x[0:rows, 0:lanes.stop - lanes.start]

    @pl.when(blk == 0)
    def _():
        loss_out[...] = loss[...]
        for p in range(REL_ROWS // LANES):
            for c in range(4):
                put(rel_out, c, slice(LANES * p, min(LANES * (p + 1), count)), jnp.transpose(rel[LANES * p:LANES * (p + 1), cols_of(c)]))

    for j in range(cols // LANES):
        at = pl.multiple_of(blk * cols + j * LANES, LANES)
        lanes = slice(LANES * j, LANES * (j + 1))
        here = pieces(at, LANES)
        for c in range(4):
            turned = jnp.transpose(ent[here[c], :])
            put(table, c, lanes, turned)
            if c == 1:
                state[j:j + 1, :] = turned[LANES - 1:LANES, :]


def solution(mesh):
    devs = mesh.shape["ent"]
    row_spec = P(("sweep", "ent"), None)
    state_spec = P(("sweep", "ent"))
    rel_spec = P("sweep", None)
    edge_spec = P(("sweep", "ent"), None, None)
    in_vmem = pl.BlockSpec(memory_space=VMEM)
    in_smem = pl.BlockSpec(memory_space=SMEM)
    in_any = pl.BlockSpec(memory_space=pl.ANY)
    hold = lambda x: pltpu.with_memory_space_constraint(x, VMEM)
    DMA = pltpu.SemaphoreType.DMA

    def per_device(ent_part, ada_part, rel_table, head_idx, tail_idx, rel_idx, neg_idx, edge_mask):
        rows, emb_dim = ent_part.shape
        rounds, edges = head_idx.shape[1:]
        negs = neg_idx.shape[2]
        chunks = edges // CHUNK
        total = 2 * edges + negs
        table_vmem = VMEM((rows * 4, LANES), F32)
        rel_vmem = VMEM((REL_ROWS, 4 * LANES), F32)
        loss_vmem = VMEM((8, LANES), F32)
        block = min(1024, rows)
        by_round = lambda x: x.transpose(1, 0, 2)
        head_idx, tail_idx, rel_idx, neg_idx, edge_mask = map(by_round, (head_idx, tail_idx, rel_idx, neg_idx, edge_mask))
        table_spec = pl.BlockSpec((emb_dim, block), lambda i: (0, i))
        ada_spec = pl.BlockSpec((block // LANES, LANES), lambda i: (i, 0))

        tail_got, neg_got, mask_got = pl.pallas_call(
            functools.partial(swap_kernel, devs),
            out_shape=tuple(jax.ShapeDtypeStruct(x.shape, x.dtype) for x in (tail_idx, neg_idx, edge_mask)),
            in_specs=[in_any] * 3,
            out_specs=(in_any,) * 3,
            scratch_shapes=[DMA((rounds, 3)), DMA((rounds, 3))],
            compiler_params=pltpu.CompilerParams(collective_id=rounds, has_side_effects=True, vmem_limit_bytes=1 << 20),
            name="swap",
        )(tail_idx, neg_idx, edge_mask)
        ent, rel, loss = pl.pallas_call(
            enter_kernel,
            grid=(rows // block,),
            out_shape=(table_vmem, rel_vmem, loss_vmem),
            in_specs=[table_spec, ada_spec, in_vmem],
            out_specs=(in_vmem,) * 3,
            scratch_shapes=[VMEM((LANES, LANES), F32)],
            compiler_params=pltpu.CompilerParams(vmem_limit_bytes=25 << 20),
            name="enter",
        )(ent_part.T, ada_part.reshape(rows // LANES, LANES), rel_table.T)

        wire = VMEM((chunks, 3 * CHUNK + SUB, LANES), BF16)
        full = VMEM((edges, 4 * LANES), F32)
        some = VMEM((CHUNK, 4 * LANES), F32)
        half_rel = (REL_ROWS // 2, 4 * LANES)
        lists = [SMEM((1, edges), jnp.int32), SMEM((1, edges), jnp.int32), SMEM((1, negs), jnp.int32)]
        for step in range(rounds):
            grads, rel, loss = pl.pallas_call(
                functools.partial(main_kernel, step, devs, emb_dim),
                out_shape=(VMEM((total * 4, LANES), F32), rel_vmem, loss_vmem),
                in_specs=[in_smem] * 3 + [in_vmem] * 8,
                out_specs=(in_vmem,) * 3,
                scratch_shapes=[
                    VMEM((4 * SUB, LANES), F32), VMEM((REL_ROWS, 12 * LANES), BF16), full, full,
                    VMEM((edges + negs, 4 * LANES), BF16), wire, wire, wire, wire,
                    VMEM((CHUNK, 4 * LANES), BF16), VMEM((CHUNK, LANES), F32), VMEM((CHUNK, negs), F32),
                    VMEM((CHUNK, 1), F32), VMEM((CHUNK, 1), F32), VMEM((CHUNK, negs), BF16), some,
                    VMEM((edges + negs, 4 * LANES), F32), some, VMEM((CHUNK, 12 * LANES), BF16), VMEM((LANES, 12 * LANES), BF16),
                    VMEM((REL_ROWS, 4 * LANES), F32), VMEM(half_rel, F32), VMEM(half_rel, BF16), VMEM(half_rel, BF16), VMEM(half_rel, BF16), VMEM(half_rel, BF16),
                    VMEM((REL_ROWS, 4 * LANES), F32), VMEM((8, LANES), F32), VMEM((8, LANES), F32),
                ] + [DMA((chunks,))] * 4 + [DMA((7,))] * 2,
                compiler_params=pltpu.CompilerParams(collective_id=step, has_side_effects=True, vmem_limit_bytes=25 << 20),
                name="train",
            )(head_idx, tail_got, neg_got, head_idx, tail_got, neg_got, mask_got, rel_idx, hold(loss), hold(rel), hold(ent.reshape(rows, 4, LANES)))
            ent = pl.pallas_call(
                functools.partial(scatter_kernel, step, emb_dim),
                out_shape=table_vmem,
                in_specs=[in_any] * 3 + [in_vmem] * 2,
                out_specs=in_vmem,
                input_output_aliases={4: 0},
                scratch_shapes=[VMEM((rows * 4, LANES), F32), VMEM((1024, LANES), F32)] + lists + [DMA((3,))],
                compiler_params=pltpu.CompilerParams(vmem_limit_bytes=18 << 20),
                name="scatter",
            )(head_idx, tail_got, neg_got, hold(grads), hold(ent))

        table_t, state, rel_t, loss = pl.pallas_call(
            functools.partial(leave_kernel, emb_dim),
            grid=(rows // block,),
            out_shape=(jax.ShapeDtypeStruct((emb_dim, rows), F32), jax.ShapeDtypeStruct((rows // LANES, LANES), F32),
                       jax.ShapeDtypeStruct(rel_table.T.shape, F32), jax.ShapeDtypeStruct((8, LANES), F32)),
            in_specs=[in_vmem] * 3,
            out_specs=(table_spec, ada_spec, in_vmem, in_vmem),
            compiler_params=pltpu.CompilerParams(vmem_limit_bytes=25 << 20),
            name="leave",
        )(hold(ent), hold(rel), hold(loss))
        return table_t.T, state.reshape(rows), rel_t.T, loss[0:1, 0:rounds]

    return jax.shard_map(per_device, mesh=mesh, in_specs=(row_spec, state_spec, rel_spec, edge_spec, edge_spec, edge_spec, edge_spec, edge_spec), out_specs=(row_spec, state_spec, rel_spec, row_spec), check_vma=False)
```

```python
import functools

import jax
import jax.numpy as jnp
from jax import lax
from jax.experimental import pallas as pl
from jax.experimental.pallas import tpu as pltpu
from jax.sharding import PartitionSpec as P

LEARN_RATE = 0.25
ADA_EPS = 1e-10
LANES = 128
SUB = 32
CHUNK = 256
REL_ROWS = 256
VMEM = pltpu.VMEM
SMEM = pltpu.SMEM
F32 = jnp.float32
BF16 = jnp.bfloat16


def lane_iota(rows):
    return lax.broadcasted_iota(jnp.int32, (rows, LANES), 1)


def updated(e, a, emb_dim, lane):
    squares = (a[0] * a[0] + a[1] * a[1]) + (a[2] * a[2] + a[3] * a[3])
    state = jnp.sum(squares * (1.0 / emb_dim) + jnp.where(lane == LANES - 1, e[1], 0.0), axis=1, keepdims=True)
    scale = LEARN_RATE * lax.rsqrt(state + ADA_EPS)
    new = [e[c] - scale * a[c] for c in range(4)]
    new[1] = jnp.where(lane == LANES - 1, state, new[1])
    return new


def split3(x):
    hi = x.astype(BF16)
    rest = x - hi.astype(F32)
    mid = rest.astype(BF16)
    return hi, mid, (rest - mid.astype(F32)).astype(BF16)


def write_wire(buf, n, b, x, short, left, lane):
    base = b * SUB
    turned = pltpu.roll(x[3], short, axis=1)
    over = 2 * short - LANES
    rows = lambda part: pl.ds(pl.multiple_of(part * CHUNK + base, SUB), SUB)
    buf[n, rows(0), :] = x[0].astype(BF16)
    buf[n, rows(1), :] = x[2].astype(BF16)
    buf[n, rows(2), :] = jnp.where(lane < short, x[1], turned).astype(BF16)
    return left + pltpu.roll(jnp.where(lane < over, turned, 0.0), b * over, axis=1)


def read_wire(buf, n, b, short, left, lane):
    base = b * SUB
    rows = lambda part: pl.ds(pl.multiple_of(part * CHUNK + base, SUB), SUB)
    over = 2 * short - LANES
    x0 = buf[n, rows(0), :].astype(F32)
    x2 = buf[n, rows(1), :].astype(F32)
    mixed = buf[n, rows(2), :].astype(F32)
    x1 = jnp.where(lane < short, mixed, 0.0)
    kept = LANES - short
    tail = pltpu.roll(left, lax.rem(LANES + kept - b * over, LANES), axis=1)
    x3 = jnp.where(lane < kept, pltpu.roll(mixed, kept, axis=1), jnp.where(lane < short, tail, 0.0))
    return [x0, x1, x2, x3]


def pieces(first, count):
    return [pl.ds(first * 4 + c, count, stride=4) for c in range(4)]


def row_of(r):
    return pl.ds(pl.multiple_of(r * 4, 4), 4)


def cols_of(c):
    return slice(LANES * c, LANES * (c + 1))


def gather_rows(ent, idx, step, start, rows):
    for i in range(SUB):
        r = idx[step, 0, start + i]
        rows[4 * i:4 * i + 4, :] = ent[r]
    return [rows[s, :] for s in pieces(0, SUB)]


def dense_update(ent, acc, states, emb_dim):
    lane = lane_iota(SUB)
    rows = states.shape[0]

    def block(o, carry):
        def measure(j, c):
            here = pieces(pl.multiple_of(o * rows + j * SUB, SUB), SUB)
            a = [acc[s, :] for s in here]
            squares = (a[0] * a[0] + a[1] * a[1]) + (a[2] * a[2] + a[3] * a[3])
            state = jnp.sum(squares * (1.0 / emb_dim) + jnp.where(lane == LANES - 1, ent[here[1], :], 0.0), axis=1, keepdims=True)
            states[pl.ds(pl.multiple_of(j * SUB, SUB), SUB), :] = jnp.broadcast_to(state, (SUB, LANES))
            return c

        def apply(j, c):
            here = pieces(pl.multiple_of(o * rows + j * SUB, SUB), SUB)
            state = states[pl.ds(pl.multiple_of(j * SUB, SUB), SUB), :]
            scale = LEARN_RATE * lax.rsqrt(state + ADA_EPS)
            for k in range(4):
                new = ent[here[k], :] - scale * acc[here[k], :]
                ent[here[k], :] = jnp.where(lane == LANES - 1, state, new) if k == 1 else new
            return c

        lax.fori_loop(0, rows // SUB, measure, 0, unroll=32)
        lax.fori_loop(0, rows // SUB, apply, 0, unroll=16)
        return carry

    lax.fori_loop(0, ent.shape[0] // (4 * rows), block, 0)


def merge_repeats(src, at, ids, split, grads, out):
    for p in range(LANES // SUB):
        part = pl.ds(pl.multiple_of(at + p * SUB, SUB), SUB)
        for c in range(4):
            for k, piece in enumerate(split3(src[part, cols_of(c)])):
                split[p * SUB:(p + 1) * SUB, 512 * k + LANES * c:512 * k + LANES * (c + 1)] = piece
    row = jnp.broadcast_to(ids, (LANES, LANES))
    i0 = lax.broadcasted_iota(jnp.int32, (LANES, LANES), 0)
    i1 = lane_iota(LANES)
    same = (jnp.transpose(row) == row) & (i1 <= i0) & (i1 // SUB == i0 // SUB)
    got = jnp.dot(jnp.where(same, 1.0, 0.0).astype(BF16), split[...], preferred_element_type=F32)
    here = pieces(out, LANES)
    for c in range(4):
        grads[here[c], :] = (got[:, cols_of(c)] + got[:, 512 + LANES * c:512 + LANES * (c + 1)]) + got[:, 1024 + LANES * c:1024 + LANES * (c + 1)]


def main_kernel(step, devs, emb_dim, head_idx, tail_idx, neg_idx, head_row, tail_row, neg_row, mask_row, rel_row, loss_in, rel_in, ent,
                grads, rel_out, loss_out,
                rows, rel_split, heads, rels, served, q_send, q_recv, dq_send, dq_recv, q_all, weights, scores,
                pos, d_pos, probs, d_mix, flat, d_head, d_split, m_split, rel_acc, rel_got, rel_half, rel_got1, rel_two, rel_got2, rel_sum,
                loss_send, loss_recv, q_ss, q_rs, d_ss, d_rs, r_ss, r_rs):
    edges = head_idx.shape[2]
    negs = neg_idx.shape[2]
    chunks = edges // CHUNK
    subs = CHUNK // SUB
    half = emb_dim // 2
    short = half - LANES
    score_scale = emb_dim ** -0.5
    shift = step + 1
    me = lax.axis_index("ent")
    owner = lax.rem(me + shift, devs)
    asker = lax.rem(me + devs - shift, devs)
    core = lax.rem(me, 2)
    x_at = lax.rem(me // 2, 2)
    y_at = me // 4
    mate = me + 1 - 2 * core
    x_mate = me + 2 - 4 * x_at
    y_mate = me + 4 - 8 * y_at
    lane = lane_iota(SUB)

    def copy_to(src, dst, send_sem, recv_sem, dev):
        return pltpu.make_async_remote_copy(src_ref=src, dst_ref=dst, send_sem=send_sem, recv_sem=recv_sem,
                                            device_id={"ent": dev}, device_id_type=pl.DeviceIdType.MESH)

    barrier = pltpu.get_barrier_semaphore()
    for dev in (owner, asker, mate, x_mate, y_mate):
        pl.semaphore_signal(barrier, inc=1, device_id={"ent": dev}, device_id_type=pl.DeviceIdType.MESH)
    def split_rel(j, carry):
        at = pl.ds(pl.multiple_of(j * SUB, SUB), SUB)
        for p, part in enumerate(split3(rel_in[at, :])):
            rel_split[at, 512 * p:512 * (p + 1)] = part
        return carry

    lax.fori_loop(0, REL_ROWS // SUB, split_rel, 0)
    def one_hot(n):
        ids = rel_row[step, 0:1, n * CHUNK:(n + 1) * CHUNK]
        return jnp.where(lax.broadcasted_iota(jnp.int32, (REL_ROWS, CHUNK), 0) == ids, 1.0, 0.0).astype(BF16)

    q_copies = []
    for n in range(chunks):
        picked = lax.dot_general(one_hot(n), rel_split[...], (((0,), (0,)), ((), ())), preferred_element_type=F32)
        rels[n * CHUNK:(n + 1) * CHUNK, :] = (picked[:, :512] + picked[:, 512:1024]) + picked[:, 1024:]

        def query(b, left, n=n):
            at = pl.multiple_of(n * CHUNK + b * SUB, SUB)
            h = gather_rows(ent, head_idx, step, at, rows)
            h[1] = jnp.where(lane < short, h[1], 0.0)
            r = [rels[pl.ds(at, SUB), cols_of(c)] for c in range(4)]
            r[1] = jnp.where(lane < short, r[1], 0.0)
            for c in range(4):
                heads[pl.ds(at, SUB), cols_of(c)] = h[c]
            q = [h[0] * r[0] - h[2] * r[2], h[1] * r[1] - h[3] * r[3], h[0] * r[2] + h[2] * r[0], h[1] * r[3] + h[3] * r[1]]
            return write_wire(q_send, n, b, q, short, left, lane)

        left = lax.fori_loop(0, subs, query, jnp.zeros((SUB, LANES), F32), unroll=4)
        q_send[n, 3 * CHUNK:, :] = left.astype(BF16)
        if n == 0:
            pl.semaphore_wait(barrier, 5)
        copy = copy_to(q_send.at[n], q_recv.at[n], q_ss.at[n], q_rs.at[n], owner)
        copy.start()
        q_copies.append(copy)

    def serve(idx, out):
        def one(j, carry):
            at = pl.multiple_of(j * SUB, SUB)
            t = gather_rows(ent, idx, step, at, rows)
            t[1] = jnp.where(lane < short, t[1], 0.0)
            for c in range(4):
                served[pl.ds(pl.multiple_of(out + at, SUB), SUB), cols_of(c)] = t[c].astype(BF16)
            return carry

        lax.fori_loop(0, idx.shape[2] // SUB, one, 0, unroll=4)

    serve(neg_idx, edges)
    serve(tail_idx, 0)

    loss = jnp.zeros((SUB, 1), F32)
    d_copies = []
    for n in range(chunks):
        for p in range(CHUNK // LANES):
            row = mask_row[step, 0:1, n * CHUNK + LANES * p:n * CHUNK + LANES * (p + 1)].astype(F32)
            weights[LANES * p:LANES * (p + 1), :] = jnp.transpose(jnp.broadcast_to(row, (LANES, LANES)))
        q_copies[n].wait_recv()

        def arrive(b, carry, n=n):
            at = pl.multiple_of(b * SUB, SUB)
            q = read_wire(q_recv, n, b, short, q_recv[n, 3 * CHUNK:, :].astype(F32), lane)
            t = [served[pl.ds(pl.multiple_of(n * CHUNK + at, SUB), SUB), cols_of(c)].astype(F32) for c in range(4)]
            pos[pl.ds(at, SUB), :] = score_scale * jnp.sum((q[0] * t[0] + q[1] * t[1]) + (q[2] * t[2] + q[3] * t[3]), axis=1, keepdims=True)
            for c in range(4):
                q_all[pl.ds(at, SUB), cols_of(c)] = q[c].astype(BF16)
            return carry

        lax.fori_loop(0, subs, arrive, 0, unroll=4)
        scores[...] = lax.dot_general(q_all[...], served[edges:, :], (((1,), (1,)), ((), ())), preferred_element_type=F32)

        def soft(b, total):
            at = pl.ds(pl.multiple_of(b * SUB, SUB), SUB)
            s = score_scale * scores[at, :]
            p = pos[at, :]
            w = weights[at, 0:1]
            top = jnp.maximum(p, jnp.max(s, axis=1, keepdims=True))
            e = jnp.exp(s - top)
            pe = jnp.exp(p - top)
            denom = pe + jnp.sum(e, axis=1, keepdims=True)
            d_pos[at, :] = score_scale * (w * (pe / denom - 1.0))
            probs[at, :] = ((w / denom) * e).astype(BF16)
            return total + w * (top + jnp.log(denom) - p)

        loss = lax.fori_loop(0, subs, soft, loss, unroll=4)
        d_mix[...] = jnp.dot(probs[...], served[edges:, :], preferred_element_type=F32)

        def back(b, left, n=n):
            at = pl.multiple_of(b * SUB, SUB)
            dp = d_pos[pl.ds(at, SUB), :]
            row = pl.ds(pl.multiple_of(n * CHUNK + at, SUB), SUB)
            dq = []
            for c in range(4):
                t = served[row, cols_of(c)].astype(F32)
                q = q_all[pl.ds(at, SUB), cols_of(c)].astype(F32)
                dq.append(dp * t + score_scale * d_mix[pl.ds(at, SUB), cols_of(c)])
                flat[row, cols_of(c)] = dp * q
            return write_wire(dq_send, n, b, dq, short, left, lane)

        left = lax.fori_loop(0, subs, back, jnp.zeros((SUB, LANES), F32), unroll=4)
        dq_send[n, 3 * CHUNK:, :] = left.astype(BF16)
        copy = copy_to(dq_send.at[n], dq_recv.at[n], d_ss.at[n], d_rs.at[n], asker)
        copy.start()
        d_copies.append(copy)
        part = lax.dot_general(probs[...], q_all[...], (((0,), (0,)), ((), ())), preferred_element_type=F32)
        if n == 0:
            flat[edges:, :] = part
        elif n < chunks - 1:
            flat[edges:, :] += part
        else:
            flat[edges:, :] = score_scale * (flat[edges:, :] + part)

    loss_send[...] = jnp.broadcast_to(jnp.sum(loss, axis=0, keepdims=True), (8, LANES))
    loss_copy = copy_to(loss_send, loss_recv, r_ss.at[6], r_rs.at[6], asker)
    loss_copy.start()

    def merge(ids, src_at, out):
        def one(j, carry):
            at = pl.multiple_of(j * LANES, LANES)
            merge_repeats(flat, src_at + at, ids[step, 0:1, pl.ds(at, LANES)], m_split, grads, out + at)
            return carry

        lax.fori_loop(0, ids.shape[2] // LANES, one, 0, unroll=2)

    merge(tail_row, 0, edges)
    merge(neg_row, edges, 2 * edges)

    for n in range(chunks):
        d_copies[n].wait_recv()

        def own(b, carry, n=n):
            at = pl.multiple_of(n * CHUNK + b * SUB, SUB)
            dq = read_wire(dq_recv, n, b, short, dq_recv[n, 3 * CHUNK:, :].astype(F32), lane)
            h = [heads[pl.ds(at, SUB), cols_of(c)] for c in range(4)]
            r = [rels[pl.ds(at, SUB), cols_of(c)] for c in range(4)]
            r[1] = jnp.where(lane < short, r[1], 0.0)
            dh = [dq[0] * r[0] + dq[2] * r[2], dq[1] * r[1] + dq[3] * r[3], dq[2] * r[0] - dq[0] * r[2], dq[3] * r[1] - dq[1] * r[3]]
            dr = [dq[0] * h[0] + dq[2] * h[2], dq[1] * h[1] + dq[3] * h[3], dq[2] * h[0] - dq[0] * h[2], dq[3] * h[1] - dq[1] * h[3]]
            row = pl.ds(pl.multiple_of(b * SUB, SUB), SUB)
            for c in range(4):
                d_head[row, cols_of(c)] = dh[c]
                for p, part in enumerate(split3(dr[c])):
                    d_split[row, 512 * p + LANES * c:512 * p + LANES * (c + 1)] = part
            return carry

        lax.fori_loop(0, subs, own, 0, unroll=4)
        part = jnp.dot(one_hot(n), d_split[...], preferred_element_type=F32)
        part = (part[:, :512] + part[:, 512:1024]) + part[:, 1024:]
        if n == 0:
            rel_acc[...] = part
        else:
            rel_acc[...] += part
        if n < chunks - 1:
            for p in range(CHUNK // LANES):
                at = n * CHUNK + p * LANES
                merge_repeats(d_head, p * LANES, head_row[step, 0:1, at:at + LANES], m_split, grads, at)

    hrows = REL_ROWS // 2
    qrows = hrows // 2
    mine = pl.ds(pl.multiple_of(core * hrows, hrows), hrows)
    theirs = pl.ds(pl.multiple_of((1 - core) * hrows, hrows), hrows)
    c0 = copy_to(rel_acc.at[theirs], rel_got, r_ss.at[0], r_rs.at[0], mate)
    c0.start()
    at = (chunks - 1) * CHUNK
    merge_repeats(d_head, 0, head_row[step, 0:1, at:at + LANES], m_split, grads, at)
    c0.wait_recv()
    rel_half[...] = (rel_acc[mine, :] + rel_got[...]).astype(BF16)
    first, last = pl.ds(0, qrows), pl.ds(qrows, qrows)
    c1 = copy_to(rel_half.at[first], rel_got1.at[first], r_ss.at[1], r_rs.at[1], x_mate)
    c2 = copy_to(rel_half.at[last], rel_got1.at[last], r_ss.at[2], r_rs.at[2], y_mate)
    c1.start()
    c2.start()
    for p in range(1, CHUNK // LANES):
        at = (chunks - 1) * CHUNK + p * LANES
        merge_repeats(d_head, p * LANES, head_row[step, 0:1, at:at + LANES], m_split, grads, at)
    c1.wait_recv()
    rel_two[first, :] = (rel_half[first, :].astype(F32) + rel_got1[first, :].astype(F32)).astype(BF16)
    c3 = copy_to(rel_two.at[first], rel_got2.at[first], r_ss.at[3], r_rs.at[3], y_mate)
    c3.start()
    c2.wait_recv()
    rel_two[last, :] = (rel_half[last, :].astype(F32) + rel_got1[last, :].astype(F32)).astype(BF16)
    c4 = copy_to(rel_two.at[last], rel_got2.at[last], r_ss.at[4], r_rs.at[4], x_mate)
    c4.start()
    c3.wait_recv()
    c4.wait_recv()
    rel_sum[mine, :] = rel_two[...].astype(F32) + rel_got2[...].astype(F32)
    c5 = copy_to(rel_sum.at[mine], rel_sum.at[mine], r_ss.at[5], r_rs.at[5], mate)
    c5.start()
    loss_copy.wait_recv()
    loss_out[...] = loss_in[...] + jnp.where(lane_iota(8) == step, loss_recv[...] * (1.0 / edges), 0.0)
    c5.wait_recv()

    def rel_step(j, carry):
        at = pl.ds(pl.multiple_of(j * SUB, SUB), SUB)
        new = updated([rel_in[at, cols_of(c)] for c in range(4)], [rel_sum[at, cols_of(c)] for c in range(4)], emb_dim, lane)
        for c in range(4):
            rel_out[at, cols_of(c)] = new[c]
        return carry

    lax.fori_loop(0, REL_ROWS // SUB, rel_step, 0, unroll=4)
    for copy in q_copies + d_copies + [loss_copy, c0, c1, c2, c3, c4, c5]:
        copy.wait_send()


def scatter_kernel(step, emb_dim, head_hbm, tail_hbm, neg_hbm, grads, ent_in, ent, acc, states, head_idx, tail_idx, neg_idx, sems):
    lists = ((head_hbm, head_idx), (tail_hbm, tail_idx), (neg_hbm, neg_idx))
    fetches = [pltpu.make_async_copy(src.at[step], dst, sems.at[k]) for k, (src, dst) in enumerate(lists)]
    for fetch in fetches:
        fetch.start()

    def clear(j, carry):
        acc[pl.ds(pl.multiple_of(j * 512, 512), 512), :] = jnp.zeros((512, LANES), F32)
        return carry

    lax.fori_loop(0, acc.shape[0] // 512, clear, 0)
    base = 0
    for fetch, (_, idx) in zip(fetches, lists):
        fetch.wait()

        def block(j, carry, idx=idx, base=base):
            at = j * SUB
            rows = [row_of(idx[0, at + i]) for i in range(SUB)]
            new = [acc[rows[i], :] + grads[row_of(base + at + i), :] for i in range(SUB)]
            for i in range(SUB):
                acc[rows[i], :] = new[i]
            return carry

        lax.fori_loop(0, idx.shape[1] // SUB, block, 0)
        base += idx.shape[1]
    dense_update(ent, acc, states, emb_dim)


def enter_kernel(devs, tail, neg, mask, table, state, rel, ent, rel_out, loss_out, tail_got, neg_got, mask_got, pad, ss, rs):
    blk = pl.program_id(0)
    cols = table.shape[1]
    half = table.shape[0] // 2
    short = half - LANES
    me = lax.axis_index("ent")

    def copies():
        out = []
        for s in range(tail.shape[0]):
            owner = lax.rem(me + s + 1, devs)
            for k, (src, dst) in enumerate(((tail, tail_got), (neg, neg_got), (mask, mask_got))):
                out.append(pltpu.make_async_remote_copy(src_ref=src.at[s], dst_ref=dst.at[s], send_sem=ss.at[s, k], recv_sem=rs.at[s, k],
                                                        device_id={"ent": owner}, device_id_type=pl.DeviceIdType.MESH))
        return out

    @pl.when(blk == 0)
    def _():
        barrier = pltpu.get_barrier_semaphore()
        for d in range(1, devs):
            pl.semaphore_signal(barrier, inc=1, device_id={"ent": lax.rem(me + d, devs)}, device_id_type=pl.DeviceIdType.MESH)
        pl.semaphore_wait(barrier, devs - 1)
        for copy in copies():
            copy.start()

    def piece(src, c, lanes, extra=None):
        first = (c // 2) * half
        width = lanes.stop - lanes.start
        if c % 2 == 0 and width == LANES:
            return src[first:first + LANES, lanes]
        count = LANES if c % 2 == 0 else short
        pad[...] = jnp.zeros((LANES, LANES), F32)
        pad[0:count, 0:width] = src[first + LANES * (c % 2):first + LANES * (c % 2) + count, lanes]
        if extra is not None:
            pad[LANES - 1:LANES, :] = extra
        return pad[...]

    @pl.when(blk == 0)
    def _():
        loss_out[...] = jnp.zeros_like(loss_out)
        count = rel.shape[1]
        for p in range(REL_ROWS // LANES):
            for c in range(4):
                rel_out[LANES * p:LANES * (p + 1), cols_of(c)] = jnp.transpose(piece(rel, c, slice(LANES * p, min(LANES * (p + 1), count))))

    for j in range(cols // LANES):
        lanes = slice(LANES * j, LANES * (j + 1))
        here = pieces(pl.multiple_of(blk * cols + j * LANES, LANES), LANES)
        for c in range(4):
            ent[here[c], :] = jnp.transpose(piece(table, c, lanes, state[j:j + 1, :] if c == 1 else None))

    @pl.when(blk == pl.num_programs(0) - 1)
    def _():
        for copy in copies():
            copy.wait()


def leave_kernel(emb_dim, ent, rel, loss, table, state, rel_out, loss_out):
    blk = pl.program_id(0)
    cols = table.shape[1]
    half = emb_dim // 2
    short = half - LANES
    count = rel_out.shape[1]

    def put(dst, c, lanes, x):
        first = (c // 2) * half + LANES * (c % 2)
        rows = short if c % 2 else LANES
        dst[first:first + rows, lanes] = x[0:rows, 0:lanes.stop - lanes.start]

    @pl.when(blk == 0)
    def _():
        loss_out[...] = loss[...]
        for p in range(REL_ROWS // LANES):
            for c in range(4):
                put(rel_out, c, slice(LANES * p, min(LANES * (p + 1), count)), jnp.transpose(rel[LANES * p:LANES * (p + 1), cols_of(c)]))

    for j in range(cols // LANES):
        at = pl.multiple_of(blk * cols + j * LANES, LANES)
        lanes = slice(LANES * j, LANES * (j + 1))
        here = pieces(at, LANES)
        for c in range(4):
            turned = jnp.transpose(ent[here[c], :])
            put(table, c, lanes, turned)
            if c == 1:
                state[j:j + 1, :] = turned[LANES - 1:LANES, :]


def solution(mesh):
    devs = mesh.shape["ent"]
    row_spec = P(("sweep", "ent"), None)
    state_spec = P(("sweep", "ent"))
    rel_spec = P("sweep", None)
    edge_spec = P(("sweep", "ent"), None, None)
    in_vmem = pl.BlockSpec(memory_space=VMEM)
    in_smem = pl.BlockSpec(memory_space=SMEM)
    in_any = pl.BlockSpec(memory_space=pl.ANY)
    hold = lambda x: pltpu.with_memory_space_constraint(x, VMEM)
    DMA = pltpu.SemaphoreType.DMA

    def per_device(ent_part, ada_part, rel_table, head_idx, tail_idx, rel_idx, neg_idx, edge_mask):
        rows, emb_dim = ent_part.shape
        rounds, edges = head_idx.shape[1:]
        negs = neg_idx.shape[2]
        chunks = edges // CHUNK
        total = 2 * edges + negs
        table_vmem = VMEM((rows * 4, LANES), F32)
        rel_vmem = VMEM((REL_ROWS, 4 * LANES), F32)
        loss_vmem = VMEM((8, LANES), F32)
        block = min(1024, rows)
        by_round = lambda x: x.transpose(1, 0, 2)
        head_idx, tail_idx, rel_idx, neg_idx, edge_mask = map(by_round, (head_idx, tail_idx, rel_idx, neg_idx, edge_mask))
        table_spec = pl.BlockSpec((emb_dim, block), lambda i: (0, i))
        ada_spec = pl.BlockSpec((block // LANES, LANES), lambda i: (i, 0))

        ent, rel, loss, tail_got, neg_got, mask_got = pl.pallas_call(
            functools.partial(enter_kernel, devs),
            grid=(rows // block,),
            out_shape=(table_vmem, rel_vmem, loss_vmem) + tuple(jax.ShapeDtypeStruct(x.shape, x.dtype) for x in (tail_idx, neg_idx, edge_mask)),
            in_specs=[in_any] * 3 + [table_spec, ada_spec, in_vmem],
            out_specs=(in_vmem,) * 3 + (in_any,) * 3,
            scratch_shapes=[VMEM((LANES, LANES), F32), DMA((rounds, 3)), DMA((rounds, 3))],
            compiler_params=pltpu.CompilerParams(collective_id=rounds, has_side_effects=True, vmem_limit_bytes=25 << 20),
            name="enter",
        )(tail_idx, neg_idx, edge_mask, ent_part.T, ada_part.reshape(rows // LANES, LANES), rel_table.T)

        wire = VMEM((chunks, 3 * CHUNK + SUB, LANES), BF16)
        full = VMEM((edges, 4 * LANES), F32)
        some = VMEM((CHUNK, 4 * LANES), F32)
        half_rel = (REL_ROWS // 2, 4 * LANES)
        lists = [SMEM((1, edges), jnp.int32), SMEM((1, edges), jnp.int32), SMEM((1, negs), jnp.int32)]
        for step in range(rounds):
            grads, rel, loss = pl.pallas_call(
                functools.partial(main_kernel, step, devs, emb_dim),
                out_shape=(VMEM((total * 4, LANES), F32), rel_vmem, loss_vmem),
                in_specs=[in_smem] * 3 + [in_vmem] * 8,
                out_specs=(in_vmem,) * 3,
                scratch_shapes=[
                    VMEM((4 * SUB, LANES), F32), VMEM((REL_ROWS, 12 * LANES), BF16), full, full,
                    VMEM((edges + negs, 4 * LANES), BF16), wire, wire, wire, wire,
                    VMEM((CHUNK, 4 * LANES), BF16), VMEM((CHUNK, LANES), F32), VMEM((CHUNK, negs), F32),
                    VMEM((CHUNK, 1), F32), VMEM((CHUNK, 1), F32), VMEM((CHUNK, negs), BF16), some,
                    VMEM((edges + negs, 4 * LANES), F32), some, VMEM((CHUNK, 12 * LANES), BF16), VMEM((LANES, 12 * LANES), BF16),
                    VMEM((REL_ROWS, 4 * LANES), F32), VMEM(half_rel, F32), VMEM(half_rel, BF16), VMEM(half_rel, BF16), VMEM(half_rel, BF16), VMEM(half_rel, BF16),
                    VMEM((REL_ROWS, 4 * LANES), F32), VMEM((8, LANES), F32), VMEM((8, LANES), F32),
                ] + [DMA((chunks,))] * 4 + [DMA((7,))] * 2,
                compiler_params=pltpu.CompilerParams(collective_id=step, has_side_effects=True, vmem_limit_bytes=25 << 20),
                name="train",
            )(head_idx, tail_got, neg_got, head_idx, tail_got, neg_got, mask_got, rel_idx, hold(loss), hold(rel), hold(ent.reshape(rows, 4, LANES)))
            ent = pl.pallas_call(
                functools.partial(scatter_kernel, step, emb_dim),
                out_shape=table_vmem,
                in_specs=[in_any] * 3 + [in_vmem] * 2,
                out_specs=in_vmem,
                input_output_aliases={4: 0},
                scratch_shapes=[VMEM((rows * 4, LANES), F32), VMEM((1024, LANES), F32)] + lists + [DMA((3,))],
                compiler_params=pltpu.CompilerParams(vmem_limit_bytes=18 << 20),
                name="scatter",
            )(head_idx, tail_got, neg_got, hold(grads), hold(ent))

        table_t, state, rel_t, loss = pl.pallas_call(
            functools.partial(leave_kernel, emb_dim),
            grid=(rows // block,),
            out_shape=(jax.ShapeDtypeStruct((emb_dim, rows), F32), jax.ShapeDtypeStruct((rows // LANES, LANES), F32),
                       jax.ShapeDtypeStruct(rel_table.T.shape, F32), jax.ShapeDtypeStruct((8, LANES), F32)),
            in_specs=[in_vmem] * 3,
            out_specs=(table_spec, ada_spec, in_vmem, in_vmem),
            compiler_params=pltpu.CompilerParams(vmem_limit_bytes=25 << 20),
            name="leave",
        )(hold(ent), hold(rel), hold(loss))
        return table_t.T, state.reshape(rows), rel_t.T, loss[0:1, 0:rounds]

    return jax.shard_map(per_device, mesh=mesh, in_specs=(row_spec, state_spec, rel_spec, edge_spec, edge_spec, edge_spec, edge_spec, edge_spec), out_specs=(row_spec, state_spec, rel_spec, row_spec), check_vma=False)
```
